512 devices in a mesh: seq: 128 (over x, z, y_lo), head: 4 (over y_hi, core).
Axes of the slice: x: 4, y: 8 (y_hi: 2, y_lo: 4; y = y_hi * 4 + y_lo), z: 8, core: 2. Of those that a mesh axis runs over, the one named last changes fastest.
Arguments:
- queries: bfloat16 [32768, 2048], P('seq', 'head'), may hold values from -6 to 6
- key_rows: bfloat16 [32768, 2048], P('seq', 'head'), may hold values from -6 to 6
- value_rows: bfloat16 [32768, 2048], P('seq', 'head'), may hold values from -6 to 6
- out_weight: bfloat16 [2048, 2048], P('head'), may hold values from -3 to 3
Outputs:
- layer_out: bfloat16 [32768, 2048], P('seq', 'head')
The draws below stay inside these ranges and needn't reach their ends.
All inputs are finite; a program needn't handle non-finite values.
Results may differ from the reference program's by a relative error of at most 0.012.
Values may be sent and summed in bfloat16 or wider, within the bound.
No kernel may reach another device: no remote copies, remote signals or barrier semaphores. Data moves between devices by JAX's collectives and lax.ppermute only.
A program may use at most 64 MiB of HBM per device.

```python
import jax
import jax.numpy as jnp
from jax import lax

HEADS = 16
HEAD_DIM = 128
LEAF = 256
LEVELS = 3
D = 2048
TOKENS = 32768
N_HEAD = 4


def run_mixed(key, salt):
    shared_draw = jax.random.normal(jax.random.fold_in(key, salt), (TOKENS // 8, D), jnp.float32)
    shared_rows = jnp.repeat(shared_draw, 8, axis=0)
    noise_rows = jax.random.normal(jax.random.fold_in(key, salt + 100), (TOKENS, D), jnp.float32)
    return jnp.clip(0.8 * shared_rows + 0.6 * noise_rows, -6.0, 6.0)


def draw_queries(key, part):
    base_draw = run_mixed(key, 11)
    return base_draw.astype(jnp.bfloat16)


def draw_key_rows(key, part):
    base_draw = run_mixed(key, 12)
    return base_draw.astype(jnp.bfloat16)


def steps_of(rng, extent, shards, smallest, top_value):
    def one(dim, parts):
        heights = jax.random.uniform(jax.random.fold_in(jax.random.fold_in(rng, 6), dim), (parts,), jnp.float32, smallest / len(shards), top_value / len(shards))
        return jnp.repeat(jnp.exp(heights), extent[dim] // parts).reshape((-1,) + (1,) * (len(extent) - dim - 1))

    level = one(*shards[0])
    for cut in shards[1:]:
        level = level * one(*cut)
    return level


def gaussian(own_key, extent, scale, limit, split=(), held_as=jnp.bfloat16):
    level = steps_of(own_key, extent, split, -0.22, 0.18) if split else 1.0
    array = jax.random.normal(own_key, extent, jnp.float32) * scale * level
    return jnp.minimum(jnp.maximum(array, -limit), limit).astype(held_as)


def setup_inputs(seed: int = 0) -> dict:
    keys = jax.random.split(jax.random.key(seed), 5)
    queries = draw_queries(jax.random.fold_in(keys[4], 71), 0)
    key_rows = draw_key_rows(jax.random.fold_in(keys[4], 71), 0)
    value_rows = gaussian(keys[2], (TOKENS, D), 1.0, 6.0, ((0, 128), (1, 4)))
    out_weight = gaussian(keys[3], (D, D), 0.5, 3.0, ((0, 4),))
    return dict(queries=queries, key_rows=key_rows, value_rows=value_rows, out_weight=out_weight)


def averaged(matrix, factor):
    blocks = matrix.shape[0] // factor
    folded = matrix.astype(jnp.float32).reshape(blocks, factor, matrix.shape[1])
    return jnp.mean(folded, axis=1).astype(jnp.bfloat16)


def level_attention(level_q, level_k, level_v, centred):
    blocks = level_q.shape[0] // LEAF
    padding = jnp.zeros((LEAF, level_k.shape[1]), level_k.dtype)
    padded_keys = jnp.concatenate([padding, level_k, padding], 0).reshape(blocks + 2, LEAF, HEADS, HEAD_DIM)
    padded_values = jnp.concatenate([padding, level_v, padding], 0).reshape(blocks + 2, LEAF, HEADS, HEAD_DIM)
    query_blocks = level_q.reshape(blocks, LEAF, HEADS, HEAD_DIM)
    scaling = HEAD_DIM ** -0.5

    def one_block(inputs):
        block_index, query_tile = inputs
        window_keys = lax.dynamic_slice_in_dim(padded_keys, block_index, 3, 0)
        window_values = lax.dynamic_slice_in_dim(padded_values, block_index, 3, 0)
        lower_ok = block_index > 0
        upper_ok = block_index < blocks - 1
        if centred:
            segments = jnp.stack([lower_ok, jnp.asarray(True), upper_ok])
        else:
            window_keys = jnp.concatenate([window_keys[0:1], window_keys[2:3]], 0)
            window_values = jnp.concatenate([window_values[0:1], window_values[2:3]], 0)
            segments = jnp.stack([lower_ok, upper_ok])
        usable = jnp.repeat(segments, LEAF)
        keys_flat = window_keys.reshape(-1, HEADS, HEAD_DIM).astype(jnp.float32)
        values_flat = window_values.reshape(-1, HEADS, HEAD_DIM).astype(jnp.float32)
        scores = jnp.einsum("qhd,khd->hqk", query_tile.astype(jnp.float32), keys_flat) * scaling
        scores = jnp.where(usable[None, None, :], scores, -jnp.inf)
        maxima = jnp.max(scores, axis=-1)
        weights = jnp.exp(scores - maxima[..., None]).astype(jnp.bfloat16)
        totals = jnp.sum(weights.astype(jnp.float32), axis=-1)
        numerator = jnp.einsum("hqk,khd->qhd", weights.astype(jnp.float32), values_flat)
        return maxima.T, totals.T, numerator

    maxima, totals, numerator = lax.map(one_block, (jnp.arange(blocks, dtype=jnp.int32), query_blocks))
    row_count = blocks * LEAF
    return maxima.reshape(row_count, HEADS), totals.reshape(row_count, HEADS), numerator.reshape(row_count, HEADS, HEAD_DIM)


def reference(queries, key_rows, value_rows, out_weight):
    row_count = queries.shape[0]
    results = []
    for level_index in range(LEVELS + 1):
        factor = 2 ** level_index
        if level_index == 0:
            level_q, level_k, level_v = queries, key_rows, value_rows
        else:
            level_q = averaged(queries, factor)
            level_k = averaged(key_rows, factor)
            level_v = averaged(value_rows, factor)
        maxima, totals, numerator = level_attention(level_q, level_k, level_v, level_index == 0)
        results.append((factor, maxima, totals, numerator))
    row_max = results[0][1]
    for entry in results[1:]:
        factor, maxima = entry[0], entry[1]
        spread = jnp.broadcast_to(maxima[:, None, :], (maxima.shape[0], factor, HEADS)).reshape(row_count, HEADS)
        row_max = jnp.maximum(row_max, spread)
    denominator = jnp.zeros((row_count, HEADS), jnp.float32)
    numer_all = jnp.zeros((row_count, HEADS, HEAD_DIM), jnp.float32)
    for entry in results:
        factor, maxima, totals, numerator = entry
        blocks = maxima.shape[0]
        local_max = row_max.reshape(blocks, factor, HEADS)
        weight_level = factor * jnp.exp(maxima[:, None, :] - local_max)
        denominator = denominator + (weight_level * totals[:, None, :]).reshape(row_count, HEADS)
        numer_all = numer_all + (weight_level[..., None] * numerator[:, None, :, :]).reshape(row_count, HEADS, HEAD_DIM)
    attended = (numer_all / denominator[..., None]).reshape(row_count, HEADS * HEAD_DIM).astype(jnp.bfloat16)
    group_width = HEADS * HEAD_DIM // N_HEAD
    output = jnp.zeros((row_count, HEADS * HEAD_DIM), jnp.float32)
    for group_index in range(N_HEAD):
        first_row = group_index * group_width
        partial_value = jnp.dot(attended[:, first_row:first_row + group_width], out_weight[first_row:first_row + group_width], preferred_element_type=jnp.float32).astype(jnp.bfloat16)
        partial_value = lax.optimization_barrier(partial_value)
        output = output + partial_value.astype(jnp.float32)
    return output.astype(jnp.bfloat16)
```

```python
import jax
import jax.numpy as jnp
from jax import lax
from jax.experimental import pallas as pl
from jax.experimental.pallas import tpu as pltpu
from jax.sharding import PartitionSpec as P

HEAD_DIM = 128
LEAF = 256
LOG2E = 1.4426950408889634
MIB = 1024 * 1024


def seq_permute(value, target_of):
    count = lax.axis_size("seq")
    pairs = [(i, target_of(i)) for i in range(count)]
    pairs = [(i, j) for i, j in pairs if 0 <= j < count]
    return lax.ppermute(value, "seq", pairs)


def head_permute(value, bit):
    count = lax.axis_size("head")
    return lax.ppermute(value, "head", [(i, i ^ bit) for i in range(count)])


def mean_matrix(rows, factor):
    row = lax.broadcasted_iota(jnp.int32, (rows, rows * factor), 0)
    col = lax.broadcasted_iota(jnp.int32, (rows, rows * factor), 1)
    return jnp.where(col // factor == row, 1.0 / factor, 0.0).astype(jnp.bfloat16)


def spread_mean_matrix(rows, factor):
    row = lax.broadcasted_iota(jnp.int32, (rows, rows), 0)
    col = lax.broadcasted_iota(jnp.int32, (rows, rows), 1)
    return jnp.where(col // factor == row // factor, 1.0 / factor, 0.0).astype(jnp.bfloat16)


def dot(left, right):
    return jnp.dot(left, right, preferred_element_type=jnp.float32)


def dot_t(left, right):
    return lax.dot_general(left, right, (((1,), (1,)), ((), ())), preferred_element_type=jnp.float32)


def coarse_kernel(k_ref, v_ref, one_ref, two_ref):
    half, quarter = mean_matrix(128, 2), mean_matrix(64, 4)
    for index, ref in enumerate((k_ref, v_ref)):
        value = ref[...]
        one_ref[index * 128 : (index + 1) * 128] = dot(half, value).astype(jnp.bfloat16)
        two_ref[index * 64 : (index + 1) * 64] = dot(quarter, value).astype(jnp.bfloat16)


def coarse(k, v):
    width = k.shape[1]
    return pl.pallas_call(
        coarse_kernel,
        out_shape=(
            jax.ShapeDtypeStruct((256, width), jnp.bfloat16),
            jax.ShapeDtypeStruct((128, width), jnp.bfloat16),
        ),
        compiler_params=pltpu.CompilerParams(vmem_limit_bytes=8 * MIB),
        cost_estimate=pl.CostEstimate(flops=10**8, bytes_accessed=10**6, transcendentals=0),
        name="coarse",
    )(k, v)


def pack_kernel(a_ref, b_ref, c_ref, d_ref, two_ref, three_ref):
    half = mean_matrix(32, 2)
    for index, ref in enumerate((a_ref, b_ref, c_ref, d_ref)):
        for part in range(2):
            value = ref[part * 64 : (part + 1) * 64]
            two_ref[part * 256 + index * 64 : part * 256 + (index + 1) * 64] = value
            three_ref[part * 128 + index * 32 : part * 128 + (index + 1) * 32] = dot(
                half, value
            ).astype(jnp.bfloat16)


def pack(pieces):
    width = pieces[0].shape[1]
    return pl.pallas_call(
        pack_kernel,
        out_shape=(
            jax.ShapeDtypeStruct((512, width), jnp.bfloat16),
            jax.ShapeDtypeStruct((256, width), jnp.bfloat16),
        ),
        compiler_params=pltpu.CompilerParams(vmem_limit_bytes=8 * MIB),
        cost_estimate=pl.CostEstimate(flops=10**8, bytes_accessed=10**6, transcendentals=0),
        name="pack",
    )(*pieces)


KEYS = 768 + 3 * 512


def attend_kernel(flags, q_ref, *refs):
    raw = refs[0:6]
    ones = refs[6:10]
    twos = refs[10:12]
    threes = refs[12:15]
    out_ref = refs[15]
    scores, weights, values = refs[16:19]

    def bias(index):
        return jnp.where(flags[index] > 0, 0.0, -jnp.inf)

    even = flags[6] > 0
    half = mean_matrix(128, 2)
    near = [
        dot(half, jnp.where(even, twos[0][p * 256 : (p + 1) * 256], twos[1][p * 256 : (p + 1) * 256]))
        .astype(jnp.bfloat16)
        for p in range(2)
    ]
    pieces = [
        (raw[0][...], raw[1][...], 0, None),
        (raw[2][...], raw[3][...], 0, 0),
        (raw[4][...], raw[5][...], 0, 1),
    ]
    for index, ref in enumerate(ones):
        pieces.append((ref[:128], ref[128:], 1, None if index < 2 else 2))
    for index, ref in enumerate(twos):
        pieces.append((ref[:256], ref[256:], 2, 3 + index))
    for index, ref in enumerate(threes):
        pieces.append((ref[:128], ref[128:], 3, (5, 7, 8)[index]))
    pieces.append((near[0], near[1], 3, 9))

    query = q_ref[...]
    queries = [query] + [
        dot(spread_mean_matrix(query.shape[0], 2**level), query).astype(jnp.bfloat16)
        for level in range(1, 4)
    ]
    values[:, HEAD_DIM:] = jnp.ones((KEYS, HEAD_DIM), jnp.bfloat16)
    largest = None
    start = 0
    spans = []
    for keys, vals, level, flag in pieces:
        count = keys.shape[0]
        part = dot_t(queries[level], keys)
        if flag is not None:
            part = part + bias(flag)
        scores[:, start : start + count] = part
        values[start : start + count, :HEAD_DIM] = vals
        for column in range(0, count, 128):
            piece = part[:, column : column + 128]
            largest = piece if largest is None else jnp.maximum(largest, piece)
        spans.append((start, count, level))
        start += count
    scale = LOG2E * HEAD_DIM**-0.5
    top = jnp.max(largest, axis=1, keepdims=True) * scale
    for start, count, level in spans:
        shifted = scores[:, start : start + count] * scale - (top - level)
        weights[:, start : start + count] = jnp.exp2(shifted).astype(jnp.bfloat16)
    total = dot(weights[...], values[...])
    out_ref[...] = (total[:, :HEAD_DIM] / total[:, HEAD_DIM:]).astype(jnp.bfloat16)


def attend(flags, q, tensors):
    rows, width = q.shape
    heads = width // HEAD_DIM

    def spec(value):
        return pl.BlockSpec((value.shape[0], HEAD_DIM), lambda h: (0, h))

    return pl.pallas_call(
        attend_kernel,
        grid=(heads,),
        in_specs=[pl.BlockSpec(memory_space=pltpu.SMEM), spec(q)] + [spec(t) for t in tensors],
        out_specs=spec(q),
        out_shape=jax.ShapeDtypeStruct((rows, width), jnp.bfloat16),
        scratch_shapes=[
            pltpu.VMEM((rows, KEYS), jnp.float32),
            pltpu.VMEM((rows, KEYS), jnp.bfloat16),
            pltpu.VMEM((KEYS, 2 * HEAD_DIM), jnp.bfloat16),
        ],
        compiler_params=pltpu.CompilerParams(vmem_limit_bytes=32 * MIB),
        cost_estimate=pl.CostEstimate(flops=3 * 10**9, bytes_accessed=6 * 10**6, transcendentals=0),
        name="attend",
    )(flags, q, *tensors)


def project_kernel(a_ref, b_ref, w_ref, out_ref):
    total = dot(a_ref[...], w_ref[:512]) + dot(b_ref[...], w_ref[512:])
    out_ref[...] = total.astype(out_ref.dtype)


def project(own, peer, weight, dtype, name):
    return pl.pallas_call(
        project_kernel,
        out_shape=jax.ShapeDtypeStruct((own.shape[0], weight.shape[1]), dtype),
        compiler_params=pltpu.CompilerParams(vmem_limit_bytes=12 * MIB),
        cost_estimate=pl.CostEstimate(flops=10**9, bytes_accessed=10**6, transcendentals=0),
        name=name,
    )(own, peer, weight)


def body(queries, key_rows, value_rows, out_weight):
    device = lax.axis_index("seq")
    head = lax.axis_index("head")
    lines = lax.axis_size("seq") // 4
    line = device // 4
    first_half = device % 4 < 2
    even = line % 2 == 0

    raw = []
    for by in (1, -1):
        for value in (key_rows, value_rows):
            raw.append(seq_permute(value, lambda i, by=by: i + by))
    own_one, own_two = coarse(key_rows, value_rows)

    two_pieces = [own_two] + [seq_permute(own_two, lambda i, j=j: i ^ j) for j in (1, 2, 3)]
    across = seq_permute(own_one, lambda i: i ^ 2)
    beside = seq_permute(across, lambda i: i ^ 1)
    along = lambda i: i + 4 if i % 4 < 2 else i - 4
    far_across = seq_permute(across, along)
    far_beside = seq_permute(beside, along)

    two_block, three_block = pack(two_pieces)
    two_low = seq_permute(two_block, lambda i: i + 4)
    two_high = seq_permute(two_block, lambda i: i - 4)
    three_low = seq_permute(three_block, lambda i: i + 8)
    three_high = seq_permute(three_block, lambda i: i - 8)
    three_skew = seq_permute(three_block, lambda i: i + 12 if i // 4 % 2 == 0 else i - 12)

    low2, high2 = line >= 2, line < lines - 2
    low3, high3 = line >= 3, line < lines - 3
    flags = jnp.stack(
        [
            device > 0,
            device < lax.axis_size("seq") - 1,
            jnp.where(first_half, line > 0, line < lines - 1),
            line > 0,
            line < lines - 1,
            low2,
            even,
            high2,
            jnp.where(even, high3, low3),
            jnp.where(even, line > 0, line < lines - 1),
        ]
    ).astype(jnp.int32)

    core, side = head % 2, head // 2
    width = queries.shape[1]
    blocks = out_weight.reshape(out_weight.shape[0], 2, 2, width)
    kept = lax.dynamic_index_in_dim(blocks, core, 2, keepdims=False)
    given = lax.dynamic_index_in_dim(blocks, 1 - core, 2, keepdims=False)
    taken = head_permute(given.reshape(out_weight.shape[0], 2 * width), 1)
    both = jnp.concatenate([kept, taken.reshape(kept.shape)], 0)
    weight_away = lax.dynamic_index_in_dim(both, 1 - side, 1, keepdims=False)
    weight_here = lax.dynamic_index_in_dim(both, side, 1, keepdims=False)

    tensors = [key_rows, value_rows] + raw + [across, beside, far_across, far_beside]
    tensors += [two_low, two_high, three_low, three_high, three_skew]
    attended = attend(flags, queries, tensors)
    peer = head_permute(attended, 1)
    away = project(attended, peer, weight_away, jnp.bfloat16, "project_away")
    arrived = head_permute(away, 2)
    here = project(attended, peer, weight_here, jnp.float32, "project_here")
    return (here + arrived.astype(jnp.float32)).astype(jnp.bfloat16)


def solution(mesh):
    in_specs = (P("seq", "head"), P("seq", "head"), P("seq", "head"), P("head", None))
    out_specs = P("seq", "head")
    return jax.shard_map(body, mesh=mesh, in_specs=in_specs, out_specs=out_specs, check_vma=False)
```

```python
import jax
import jax.numpy as jnp
from jax import lax
from jax.experimental import pallas as pl
from jax.experimental.pallas import tpu as pltpu
from jax.sharding import PartitionSpec as P


HEAD_DIM = 128
LOG2E = 1.4426950408889634
MIB = 1024 * 1024


def seq_permute(value, target_of):
    count = lax.axis_size("seq")
    pairs = [(i, target_of(i)) for i in range(count)]
    pairs = [(i, j) for i, j in pairs if 0 <= j < count]
    return lax.ppermute(value, "seq", pairs)


def head_permute(value, bit):
    count = lax.axis_size("head")
    return lax.ppermute(value, "head", [(i, i ^ bit) for i in range(count)])


def mean_matrix(rows, factor):
    row = lax.broadcasted_iota(jnp.int32, (rows, rows * factor), 0)
    col = lax.broadcasted_iota(jnp.int32, (rows, rows * factor), 1)
    return jnp.where(col // factor == row, 1.0 / factor, 0.0).astype(jnp.bfloat16)


def spread_mean_matrix(rows, factor):
    row = lax.broadcasted_iota(jnp.int32, (rows, rows), 0)
    col = lax.broadcasted_iota(jnp.int32, (rows, rows), 1)
    return jnp.where(col // factor == row // factor, 1.0 / factor, 0.0).astype(jnp.bfloat16)


def dot(left, right):
    return jnp.dot(left, right, preferred_element_type=jnp.float32)


def dot_t(left, right):
    return lax.dot_general(left, right, (((1,), (1,)), ((), ())), preferred_element_type=jnp.float32)


def coarse_kernel(k_ref, v_ref, raw_ref, one_ref, two_ref):
    half, quarter = mean_matrix(128, 2), mean_matrix(64, 4)
    for index, ref in enumerate((k_ref, v_ref)):
        value = ref[...]
        raw_ref[index * 256 : (index + 1) * 256] = value
        one_ref[index * 128 : (index + 1) * 128] = dot(half, value).astype(jnp.bfloat16)
        two_ref[index * 64 : (index + 1) * 64] = dot(quarter, value).astype(jnp.bfloat16)


def coarse(k, v):
    width = k.shape[1]
    return pl.pallas_call(
        coarse_kernel,
        out_shape=(
            jax.ShapeDtypeStruct((512, width), jnp.bfloat16),
            jax.ShapeDtypeStruct((256, width), jnp.bfloat16),
            jax.ShapeDtypeStruct((128, width), jnp.bfloat16),
        ),
        compiler_params=pltpu.CompilerParams(vmem_limit_bytes=8 * MIB),
        cost_estimate=pl.CostEstimate(flops=10**8, bytes_accessed=10**6, transcendentals=0),
        name="coarse",
    )(k, v)


def join_kernel(a_ref, b_ref, out_ref):
    out_ref[:128] = a_ref[...]
    out_ref[128:] = b_ref[...]


def join(a, b):
    return pl.pallas_call(
        join_kernel,
        out_shape=jax.ShapeDtypeStruct((256, a.shape[1]), a.dtype),
        compiler_params=pltpu.CompilerParams(vmem_limit_bytes=4 * MIB),
        cost_estimate=pl.CostEstimate(flops=10**8, bytes_accessed=10**6, transcendentals=0),
        name="join",
    )(a, b)


def pack_kernel(a_ref, b_ref, two_ref, three_ref):
    half = mean_matrix(32, 2)
    for index, (ref, base) in enumerate(((a_ref, 0), (a_ref, 128), (b_ref, 0), (b_ref, 128))):
        for part in range(2):
            value = ref[base + part * 64 : base + (part + 1) * 64]
            two_ref[part * 256 + index * 64 : part * 256 + (index + 1) * 64] = value
            three_ref[part * 128 + index * 32 : part * 128 + (index + 1) * 32] = dot(
                half, value
            ).astype(jnp.bfloat16)


def pack(pieces):
    width = pieces[0].shape[1]
    return pl.pallas_call(
        pack_kernel,
        out_shape=(
            jax.ShapeDtypeStruct((512, width), jnp.bfloat16),
            jax.ShapeDtypeStruct((256, width), jnp.bfloat16),
        ),
        compiler_params=pltpu.CompilerParams(vmem_limit_bytes=8 * MIB),
        cost_estimate=pl.CostEstimate(flops=10**8, bytes_accessed=10**6, transcendentals=0),
        name="pack",
    )(*pieces)


KEYS = 768 + 3 * 512


def attend_kernel(flags, q_ref, *refs):
    k_ref, v_ref, left, right = refs[0:4]
    ones = refs[4:7]
    twos = refs[7:9]
    threes = refs[9:12]
    out_ref = refs[12]
    scores, weights, values = refs[13:16]

    def bias(index):
        return jnp.where(flags[index] > 0, 0.0, -jnp.inf)

    even = flags[6] > 0
    half = mean_matrix(128, 2)
    beside_left = flags[2] > 0
    fourth = [
        dot(half, jnp.where(beside_left, left[p * 256 : (p + 1) * 256], right[p * 256 : (p + 1) * 256]))
        .astype(jnp.bfloat16)
        for p in range(2)
    ]
    near = [
        dot(half, jnp.where(even, twos[0][p * 256 : (p + 1) * 256], twos[1][p * 256 : (p + 1) * 256]))
        .astype(jnp.bfloat16)
        for p in range(2)
    ]
    pieces = [
        (k_ref[...], v_ref[...], 0, None),
        (left[:256], left[256:], 0, 0),
        (right[:256], right[256:], 0, 1),
    ]
    for index, ref in enumerate(ones):
        pieces.append((ref[:128], ref[128:], 1, (None, 10, 11)[index]))
    pieces.append((fourth[0], fourth[1], 1, 12))
    for index, ref in enumerate(twos):
        pieces.append((ref[:256], ref[256:], 2, 3 + index))
    for index, ref in enumerate(threes):
        pieces.append((ref[:128], ref[128:], 3, (5, 7, 8)[index]))
    pieces.append((near[0], near[1], 3, 9))

    query = q_ref[...]
    queries = [query] + [
        dot(spread_mean_matrix(query.shape[0], 2**level), query).astype(jnp.bfloat16)
        for level in range(1, 4)
    ]
    values[:, HEAD_DIM:] = jnp.ones((KEYS, HEAD_DIM), jnp.bfloat16)
    largest = None
    start = 0
    spans = []
    for keys, vals, level, flag in pieces:
        count = keys.shape[0]
        part = dot_t(queries[level], keys)
        if flag is not None:
            part = part + bias(flag)
        scores[:, start : start + count] = part
        values[start : start + count, :HEAD_DIM] = vals
        for column in range(0, count, 128):
            piece = part[:, column : column + 128]
            largest = piece if largest is None else jnp.maximum(largest, piece)
        spans.append((start, count, level))
        start += count
    scale = LOG2E * HEAD_DIM**-0.5
    top = jnp.max(largest, axis=1, keepdims=True) * scale
    for start, count, level in spans:
        shifted = scores[:, start : start + count] * scale - (top - level)
        weights[:, start : start + count] = jnp.exp2(shifted).astype(jnp.bfloat16)
    total = dot(weights[...], values[...])
    out_ref[...] = (total[:, :HEAD_DIM] / total[:, HEAD_DIM:]).astype(jnp.bfloat16)


def attend(flags, q, tensors):
    rows, width = q.shape
    heads = width // HEAD_DIM

    def spec(value):
        return pl.BlockSpec((value.shape[0], HEAD_DIM), lambda h: (0, h))

    return pl.pallas_call(
        attend_kernel,
        grid=(heads,),
        in_specs=[pl.BlockSpec(memory_space=pltpu.SMEM), spec(q)] + [spec(t) for t in tensors],
        out_specs=spec(q),
        out_shape=jax.ShapeDtypeStruct((rows, width), jnp.bfloat16),
        scratch_shapes=[
            pltpu.VMEM((rows, KEYS), jnp.float32),
            pltpu.VMEM((rows, KEYS), jnp.bfloat16),
            pltpu.VMEM((KEYS, 2 * HEAD_DIM), jnp.bfloat16),
        ],
        compiler_params=pltpu.CompilerParams(vmem_limit_bytes=32 * MIB),
        cost_estimate=pl.CostEstimate(flops=3 * 10**9, bytes_accessed=6 * 10**6, transcendentals=0),
        name="attend",
    )(flags, q, *tensors)


def project_kernel(column, a_ref, b_ref, wa_ref, wb_ref, out_ref):
    total = dot(a_ref[...], wa_ref[...]) + dot(b_ref[...], wb_ref[...])
    out_ref[...] = total.astype(out_ref.dtype)


def project(column, own, peer, own_weight, peer_weight, dtype):
    rows, width = own.shape
    block = pl.BlockSpec((rows, width), lambda i, c: (0, 0))
    weight = pl.BlockSpec((width, width), lambda i, c: (0, c[0]))
    return pl.pallas_call(
        project_kernel,
        grid_spec=pltpu.PrefetchScalarGridSpec(
            num_scalar_prefetch=1,
            grid=(1,),
            in_specs=[block, block, weight, weight],
            out_specs=block,
        ),
        out_shape=jax.ShapeDtypeStruct((rows, width), dtype),
        compiler_params=pltpu.CompilerParams(vmem_limit_bytes=12 * MIB),
        cost_estimate=pl.CostEstimate(flops=10**9, bytes_accessed=10**6, transcendentals=0),
    )(column, own, peer, own_weight, peer_weight)


def layer(queries, key_rows, value_rows, out_weight):
    device = lax.axis_index("seq")
    head = lax.axis_index("head")
    last = lax.axis_size("seq") - 1
    lines = lax.axis_size("seq") // 4
    line = device // 4
    spot = device % 4
    even = line % 2 == 0

    raw, own_one, own_two = coarse(key_rows, value_rows)
    two_across = seq_permute(own_two, lambda i: i ^ 2)
    across = seq_permute(own_one, lambda i: i ^ 2)
    two_half = join(own_two, two_across)
    two_beside = seq_permute(two_half, lambda i: i ^ 1)
    left = seq_permute(raw, lambda i: i + 1)
    right = seq_permute(raw, lambda i: i - 1)
    peer_weight = head_permute(out_weight, 1)

    two_block, three_block = pack((two_half, two_beside))
    two_low = seq_permute(two_block, lambda i: i + 4)
    two_high = seq_permute(two_block, lambda i: i - 4)
    three_low = seq_permute(three_block, lambda i: i + 8)
    three_high = seq_permute(three_block, lambda i: i - 8)
    three_skew = seq_permute(three_block, lambda i: i + 12 if i // 4 % 2 == 0 else i - 12)
    far = seq_permute(across, lambda i: i + 4 if i % 4 < 2 else i - 4)
    outer = (spot == 0) | (spot == 3)
    handed = jnp.where(outer, far, across)
    third = seq_permute(handed, lambda i: i ^ 1)

    far_ok = jnp.where(spot < 2, line > 0, line < lines - 1)
    flags = jnp.stack(
        [
            device > 0,
            device < last,
            spot % 2 == 0,
            line > 0,
            line < lines - 1,
            line >= 2,
            even,
            line < lines - 2,
            jnp.where(even, line < lines - 3, line >= 3),
            jnp.where(even, line > 0, line < lines - 1),
            far_ok,
            outer | far_ok,
            jnp.logical_not(outer) | far_ok,
        ]
    ).astype(jnp.int32)
    tensors = [key_rows, value_rows, left, right, across, far, third]
    tensors += [two_low, two_high, three_low, three_high, three_skew]
    attended = attend(flags, queries, tensors)
    peer = head_permute(attended, 1)
    here_column, away_column = head.reshape(1), (head ^ 2).reshape(1)
    weights = (out_weight, peer_weight)
    away = project(away_column, attended, peer, *weights, jnp.bfloat16)
    arrived = head_permute(away, 2)
    here = project(here_column, attended, peer, *weights, jnp.float32)
    return (here + arrived.astype(jnp.float32)).astype(jnp.bfloat16)


def solution(mesh):
    in_specs = (P("seq", "head"), P("seq", "head"), P("seq", "head"), P("head", None))
    out_specs = P("seq", "head")
    return jax.shard_map(layer, mesh=mesh, in_specs=in_specs, out_specs=out_specs, check_vma=False)
```

```python
import jax
import jax.numpy as jnp
from jax import lax
from jax.experimental import pallas as pl
from jax.experimental.pallas import tpu as pltpu
from jax.sharding import PartitionSpec as P


HEAD_DIM = 128
LOG2E = 1.4426950408889634
MIB = 1024 * 1024


def seq_permute(value, target_of):
    count = lax.axis_size("seq")
    pairs = [(i, target_of(i)) for i in range(count)]
    pairs = [(i, j) for i, j in pairs if 0 <= j < count]
    return lax.ppermute(value, "seq", pairs)


def head_permute(value, bit):
    count = lax.axis_size("head")
    return lax.ppermute(value, "head", [(i, i ^ bit) for i in range(count)])


def mean_matrix(rows, factor):
    row = lax.broadcasted_iota(jnp.int32, (rows, rows * factor), 0)
    col = lax.broadcasted_iota(jnp.int32, (rows, rows * factor), 1)
    return jnp.where(col // factor == row, 1.0 / factor, 0.0).astype(jnp.bfloat16)


def spread_mean_matrix(rows, factor):
    row = lax.broadcasted_iota(jnp.int32, (rows, rows), 0)
    col = lax.broadcasted_iota(jnp.int32, (rows, rows), 1)
    return jnp.where(col // factor == row // factor, 1.0 / factor, 0.0).astype(jnp.bfloat16)


def dot(left, right):
    return jnp.dot(left, right, preferred_element_type=jnp.float32)


def dot_t(left, right):
    return lax.dot_general(left, right, (((1,), (1,)), ((), ())), preferred_element_type=jnp.float32)


def coarse_kernel(k_ref, v_ref, raw_ref, one_ref, two_ref):
    half, quarter = mean_matrix(128, 2), mean_matrix(64, 4)
    for index, ref in enumerate((k_ref, v_ref)):
        value = ref[...]
        raw_ref[index * 256 : (index + 1) * 256] = value
        one_ref[index * 128 : (index + 1) * 128] = dot(half, value).astype(jnp.bfloat16)
        two_ref[index * 64 : (index + 1) * 64] = dot(quarter, value).astype(jnp.bfloat16)


def coarse(k, v):
    width = k.shape[1]
    return pl.pallas_call(
        coarse_kernel,
        out_shape=(
            jax.ShapeDtypeStruct((512, width), jnp.bfloat16),
            jax.ShapeDtypeStruct((256, width), jnp.bfloat16),
            jax.ShapeDtypeStruct((128, width), jnp.bfloat16),
        ),
        compiler_params=pltpu.CompilerParams(vmem_limit_bytes=8 * MIB),
        cost_estimate=pl.CostEstimate(flops=10**8, bytes_accessed=10**6, transcendentals=0),
        name="coarse",
    )(k, v)


def half_kernel(two_ref, one_ref, out_ref):
    half = mean_matrix(64, 2)
    for part in range(2):
        base = part * 128
        out_ref[base : base + 64] = two_ref[part * 64 : (part + 1) * 64]
        out_ref[base + 64 : base + 128] = dot(half, one_ref[base : base + 128]).astype(jnp.bfloat16)


def halve_kernel(a_ref, b_ref, out_ref):
    half = mean_matrix(64, 2)
    for part in range(2):
        base = part * 128
        for index, ref in enumerate((a_ref, b_ref)):
            start = base + index * 64
            out_ref[start : start + 64] = dot(half, ref[base : base + 128]).astype(jnp.bfloat16)


def small(kernel, a, b):
    return pl.pallas_call(
        kernel,
        out_shape=jax.ShapeDtypeStruct((256, a.shape[1]), a.dtype),
        compiler_params=pltpu.CompilerParams(vmem_limit_bytes=4 * MIB),
        cost_estimate=pl.CostEstimate(flops=10**8, bytes_accessed=10**6, transcendentals=0),
    )(a, b)


KEYS = 768 + 3 * 512


def attend_kernel(flags, q_ref, *refs):
    k_ref, v_ref, left, right = refs[0:4]
    ones = refs[4:7]
    twos = refs[7:11]
    threes = refs[11:14]
    nears = refs[14:16]
    out_ref = refs[16]
    scores, weights, values = refs[17:20]

    def bias(index):
        return jnp.where(flags[index] > 0, 0.0, -jnp.inf)

    even = flags[6] > 0
    half = mean_matrix(128, 2)
    beside_left = flags[2] > 0
    fourth = [
        dot(half, jnp.where(beside_left, left[p * 256 : (p + 1) * 256], right[p * 256 : (p + 1) * 256]))
        .astype(jnp.bfloat16)
        for p in range(2)
    ]
    near = [
        jnp.where(even, nears[0][p * 128 : (p + 1) * 128], nears[1][p * 128 : (p + 1) * 128])
        for p in range(2)
    ]
    pieces = [
        (k_ref[...], v_ref[...], 0, None),
        (left[:256], left[256:], 0, 0),
        (right[:256], right[256:], 0, 1),
    ]
    for index, ref in enumerate(ones):
        pieces.append((ref[:128], ref[128:], 1, (None, 10, 11)[index]))
    pieces.append((fourth[0], fourth[1], 1, 12))
    for index, ref in enumerate(twos):
        pieces.append((ref[:128], ref[128:], 2, 3 + index // 2))
    for index, ref in enumerate(threes):
        pieces.append((ref[:128], ref[128:], 3, (5, 7, 8)[index]))
    pieces.append((near[0], near[1], 3, 9))

    query = q_ref[...]
    queries = [query] + [
        dot(spread_mean_matrix(query.shape[0], 2**level), query).astype(jnp.bfloat16)
        for level in range(1, 4)
    ]
    values[:, HEAD_DIM:] = jnp.ones((KEYS, HEAD_DIM), jnp.bfloat16)
    largest = None
    start = 0
    spans = []
    for keys, vals, level, flag in pieces:
        count = keys.shape[0]
        part = dot_t(queries[level], keys)
        if flag is not None:
            part = part + bias(flag)
        scores[:, start : start + count] = part
        values[start : start + count, :HEAD_DIM] = vals
        for column in range(0, count, 128):
            piece = part[:, column : column + 128]
            largest = piece if largest is None else jnp.maximum(largest, piece)
        spans.append((start, count, level))
        start += count
    scale = LOG2E * HEAD_DIM**-0.5
    top = jnp.max(largest, axis=1, keepdims=True) * scale
    for start, count, level in spans:
        shifted = scores[:, start : start + count] * scale - (top - level)
        weights[:, start : start + count] = jnp.exp2(shifted).astype(jnp.bfloat16)
    total = dot(weights[...], values[...])
    out_ref[...] = (total[:, :HEAD_DIM] / total[:, HEAD_DIM:]).astype(jnp.bfloat16)


def attend(flags, q, tensors):
    rows, width = q.shape
    heads = width // HEAD_DIM

    def spec(value):
        return pl.BlockSpec((value.shape[0], HEAD_DIM), lambda h: (0, h))

    return pl.pallas_call(
        attend_kernel,
        grid=(heads,),
        in_specs=[pl.BlockSpec(memory_space=pltpu.SMEM), spec(q)] + [spec(t) for t in tensors],
        out_specs=spec(q),
        out_shape=jax.ShapeDtypeStruct((rows, width), jnp.bfloat16),
        scratch_shapes=[
            pltpu.VMEM((rows, KEYS), jnp.float32),
            pltpu.VMEM((rows, KEYS), jnp.bfloat16),
            pltpu.VMEM((KEYS, 2 * HEAD_DIM), jnp.bfloat16),
        ],
        compiler_params=pltpu.CompilerParams(vmem_limit_bytes=32 * MIB),
        cost_estimate=pl.CostEstimate(flops=3 * 10**9, bytes_accessed=6 * 10**6, transcendentals=0),
        name="attend",
    )(flags, q, *tensors)


def project_kernel(column, a_ref, b_ref, wa_ref, wb_ref, out_ref):
    total = dot(a_ref[...], wa_ref[...]) + dot(b_ref[...], wb_ref[...])
    out_ref[...] = total.astype(out_ref.dtype)


def project(column, own, peer, own_weight, peer_weight, dtype):
    rows, width = own.shape
    block = pl.BlockSpec((rows, width), lambda i, c: (0, 0))
    weight = pl.BlockSpec((width, width), lambda i, c: (0, c[0]))
    return pl.pallas_call(
        project_kernel,
        grid_spec=pltpu.PrefetchScalarGridSpec(
            num_scalar_prefetch=1,
            grid=(1,),
            in_specs=[block, block, weight, weight],
            out_specs=block,
        ),
        out_shape=jax.ShapeDtypeStruct((rows, width), dtype),
        compiler_params=pltpu.CompilerParams(vmem_limit_bytes=12 * MIB),
        cost_estimate=pl.CostEstimate(flops=10**9, bytes_accessed=10**6, transcendentals=0),
    )(column, own, peer, own_weight, peer_weight)


def layer(queries, key_rows, value_rows, out_weight):
    device = lax.axis_index("seq")
    head = lax.axis_index("head")
    last = lax.axis_size("seq") - 1
    lines = lax.axis_size("seq") // 4
    line = device // 4
    spot = device % 4
    even = line % 2 == 0

    raw, own_one, own_two = coarse(key_rows, value_rows)
    across = seq_permute(own_one, lambda i: i ^ 2)
    two_half = small(half_kernel, own_two, across)
    two_beside = seq_permute(two_half, lambda i: i ^ 1)
    low_a = seq_permute(two_half, lambda i: i + 4)
    high_a = seq_permute(two_half, lambda i: i - 4)
    far = seq_permute(across, lambda i: i + 4 if i % 4 < 2 else i - 4)
    left = seq_permute(raw, lambda i: i + 1)
    right = seq_permute(raw, lambda i: i - 1)
    low_b = seq_permute(two_beside, lambda i: i + 4)
    high_b = seq_permute(two_beside, lambda i: i - 4)
    three_block = small(halve_kernel, two_half, two_beside)
    three_skew = seq_permute(three_block, lambda i: i + 12 if i // 4 % 2 == 0 else i - 12)
    peer_weight = head_permute(out_weight, 1)
    outer = (spot == 0) | (spot == 3)
    handed = jnp.where(outer, far, across)
    third = seq_permute(handed, lambda i: i ^ 1)
    near_low = small(halve_kernel, low_a, low_b)
    near_high = small(halve_kernel, high_a, high_b)
    three_low = seq_permute(near_low, lambda i: i + 4)
    three_high = seq_permute(near_high, lambda i: i - 4)

    far_ok = jnp.where(spot < 2, line > 0, line < lines - 1)
    flags = jnp.stack(
        [
            device > 0,
            device < last,
            spot % 2 == 0,
            line > 0,
            line < lines - 1,
            line >= 2,
            even,
            line < lines - 2,
            jnp.where(even, line < lines - 3, line >= 3),
            jnp.where(even, line > 0, line < lines - 1),
            far_ok,
            outer | far_ok,
            jnp.logical_not(outer) | far_ok,
        ]
    ).astype(jnp.int32)
    tensors = [key_rows, value_rows, left, right, across, far, third]
    tensors += [low_a, low_b, high_a, high_b, three_low, three_high, three_skew]
    tensors += [near_low, near_high]
    tensors = [pltpu.with_memory_space_constraint(t, pltpu.HBM) for t in tensors]
    own_queries = pltpu.with_memory_space_constraint(queries, pltpu.HBM)
    attended = attend(flags, own_queries, tensors)
    peer = head_permute(attended, 1)
    here_column, away_column = head.reshape(1), (head ^ 2).reshape(1)
    weights = (out_weight, peer_weight)
    away = project(away_column, attended, peer, *weights, jnp.bfloat16)
    arrived = head_permute(away, 2)
    here = project(here_column, attended, peer, *weights, jnp.float32)
    return (here + arrived.astype(jnp.float32)).astype(jnp.bfloat16)


def solution(mesh):
    in_specs = (P("seq", "head"), P("seq", "head"), P("seq", "head"), P("head", None))
    out_specs = P("seq", "head")
    return jax.shard_map(layer, mesh=mesh, in_specs=in_specs, out_specs=out_specs, check_vma=False)
```

```python
import jax
import jax.numpy as jnp
from jax import lax
from jax.experimental import pallas as pl
from jax.experimental.pallas import tpu as pltpu
from jax.sharding import PartitionSpec as P


HEAD_DIM = 128
LOG2E = 1.4426950408889634
MIB = 1024 * 1024


def seq_permute(value, target_of):
    count = lax.axis_size("seq")
    pairs = [(i, target_of(i)) for i in range(count)]
    pairs = [(i, j) for i, j in pairs if 0 <= j < count]
    return lax.ppermute(value, "seq", pairs)


def head_permute(value, bit):
    count = lax.axis_size("head")
    return lax.ppermute(value, "head", [(i, i ^ bit) for i in range(count)])


def mean_matrix(rows, factor):
    row = lax.broadcasted_iota(jnp.int32, (rows, rows * factor), 0)
    col = lax.broadcasted_iota(jnp.int32, (rows, rows * factor), 1)
    return jnp.where(col // factor == row, 1.0 / factor, 0.0).astype(jnp.bfloat16)


def spread_mean_matrix(rows, factor):
    row = lax.broadcasted_iota(jnp.int32, (rows, rows), 0)
    col = lax.broadcasted_iota(jnp.int32, (rows, rows), 1)
    return jnp.where(col // factor == row // factor, 1.0 / factor, 0.0).astype(jnp.bfloat16)


def dot(left, right):
    return jnp.dot(left, right, preferred_element_type=jnp.float32)


def dot_t(left, right):
    return lax.dot_general(left, right, (((1,), (1,)), ((), ())), preferred_element_type=jnp.float32)


def coarse_kernel(k_ref, v_ref, raw_ref, one_ref, two_ref):
    half, quarter = mean_matrix(128, 2), mean_matrix(64, 4)
    for index, ref in enumerate((k_ref, v_ref)):
        value = ref[...]
        raw_ref[index * 256 : (index + 1) * 256] = value
        one_ref[index * 128 : (index + 1) * 128] = dot(half, value).astype(jnp.bfloat16)
        two_ref[index * 64 : (index + 1) * 64] = dot(quarter, value).astype(jnp.bfloat16)


def coarse(k, v):
    width = k.shape[1]
    return pl.pallas_call(
        coarse_kernel,
        out_shape=(
            jax.ShapeDtypeStruct((512, width), jnp.bfloat16),
            jax.ShapeDtypeStruct((256, width), jnp.bfloat16),
            jax.ShapeDtypeStruct((128, width), jnp.bfloat16),
        ),
        compiler_params=pltpu.CompilerParams(vmem_limit_bytes=8 * MIB),
        cost_estimate=pl.CostEstimate(flops=10**8, bytes_accessed=10**6, transcendentals=0),
        name="coarse",
    )(k, v)


def half_kernel(two_ref, one_ref, out_ref):
    half = mean_matrix(64, 2)
    for part in range(2):
        base = part * 128
        out_ref[base : base + 64] = two_ref[part * 64 : (part + 1) * 64]
        out_ref[base + 64 : base + 128] = dot(half, one_ref[base : base + 128]).astype(jnp.bfloat16)


def halve_kernel(block_ref, out_ref):
    half = mean_matrix(128, 2)
    for part in range(2):
        out_ref[part * 128 : (part + 1) * 128] = dot(
            half, block_ref[part * 256 : (part + 1) * 256]
        ).astype(jnp.bfloat16)


def pack_kernel(a_ref, b_ref, two_ref, three_ref):
    half = mean_matrix(64, 2)
    for part in range(2):
        for index, ref in enumerate((a_ref, b_ref)):
            value = ref[part * 128 : (part + 1) * 128]
            start = part * 256 + index * 128
            two_ref[start : start + 128] = value
            three_ref[start // 2 : start // 2 + 64] = dot(half, value).astype(jnp.bfloat16)


def small(kernel, *operands, rows=(256,)):
    width, dtype = operands[0].shape[1], operands[0].dtype
    shapes = tuple(jax.ShapeDtypeStruct((count, width), dtype) for count in rows)
    return pl.pallas_call(
        kernel,
        out_shape=shapes if len(rows) > 1 else shapes[0],
        compiler_params=pltpu.CompilerParams(vmem_limit_bytes=4 * MIB),
        cost_estimate=pl.CostEstimate(flops=10**8, bytes_accessed=10**6, transcendentals=0),
    )(*operands)


LATE = 2 * 128
KEYS = 768 + 3 * 512 - LATE
SCALE = LOG2E * HEAD_DIM**-0.5


def bias(flags, index):
    return jnp.where(flags[index] > 0, 0.0, -jnp.inf)


def main_kernel(flags, q_ref, *refs):
    k_ref, v_ref, left, right = refs[0:4]
    ones = refs[4:7]
    twos = refs[7:9]
    skew = refs[9]
    nears = refs[10:12]
    sum_ref, weight_ref, top_ref = refs[12:15]
    scores, weights, values = refs[15:18]

    even = flags[6] > 0
    half = mean_matrix(128, 2)
    beside_left = flags[2] > 0
    fourth = [
        dot(half, jnp.where(beside_left, left[p * 256 : (p + 1) * 256], right[p * 256 : (p + 1) * 256]))
        .astype(jnp.bfloat16)
        for p in range(2)
    ]
    near = [
        jnp.where(even, nears[0][p * 128 : (p + 1) * 128], nears[1][p * 128 : (p + 1) * 128])
        for p in range(2)
    ]
    pieces = [
        (k_ref[...], v_ref[...], 0, None),
        (left[:256], left[256:], 0, 0),
        (right[:256], right[256:], 0, 1),
    ]
    for index, ref in enumerate(ones):
        pieces.append((ref[:128], ref[128:], 1, (None, 10, 11)[index]))
    pieces.append((fourth[0], fourth[1], 1, 12))
    for index, ref in enumerate(twos):
        pieces.append((ref[:256], ref[256:], 2, 3 + index))
    pieces.append((skew[:128], skew[128:], 3, 8))
    pieces.append((near[0], near[1], 3, 9))

    query = q_ref[...]
    queries = [query] + [
        dot(spread_mean_matrix(query.shape[0], 2**level), query).astype(jnp.bfloat16)
        for level in range(1, 4)
    ]
    values[:, HEAD_DIM:] = jnp.ones((KEYS, HEAD_DIM), jnp.bfloat16)
    largest = None
    start = 0
    spans = []
    for keys, vals, level, flag in pieces:
        count = keys.shape[0]
        part = dot_t(queries[level], keys)
        if flag is not None:
            part = part + bias(flags, flag)
        scores[:, start : start + count] = part
        values[start : start + count, :HEAD_DIM] = vals
        for column in range(0, count, 128):
            piece = part[:, column : column + 128]
            largest = piece if largest is None else jnp.maximum(largest, piece)
        spans.append((start, count, level))
        start += count
    top = jnp.max(largest, axis=1, keepdims=True) * SCALE
    for start, count, level in spans:
        shifted = scores[:, start : start + count] * SCALE - (top - level)
        weights[:, start : start + count] = jnp.exp2(shifted).astype(jnp.bfloat16)
    total = dot(weights[...], values[...])
    sum_ref[...] = total[:, :HEAD_DIM]
    weight_ref[...] = total[:, HEAD_DIM:]
    top_ref[...] = jnp.broadcast_to(top, top_ref.shape)


def late_kernel(flags, q_ref, sum_ref, weight_ref, top_ref, low, high, out_ref, values):
    query = q_ref[...]
    query = dot(spread_mean_matrix(query.shape[0], 8), query).astype(jnp.bfloat16)
    values[:, HEAD_DIM:] = jnp.ones((LATE, HEAD_DIM), jnp.bfloat16)
    parts = []
    for index, (ref, flag) in enumerate(((low, 5), (high, 7))):
        parts.append(dot_t(query, ref[:128]) + bias(flags, flag))
        values[index * 128 : (index + 1) * 128, :HEAD_DIM] = ref[128:]
    early = top_ref[...]
    top = jnp.max(jnp.maximum(parts[0], parts[1]), axis=1, keepdims=True) * SCALE
    top = jnp.maximum(early, top)
    kept = jnp.exp2(early - top)
    part = jnp.concatenate([jnp.exp2(p * SCALE - (top - 3.0)) for p in parts], 1)
    total = dot(part.astype(jnp.bfloat16), values[...])
    numerator = sum_ref[...] * kept + total[:, :HEAD_DIM]
    denominator = weight_ref[...] * kept + total[:, HEAD_DIM:]
    out_ref[...] = (numerator / denominator).astype(jnp.bfloat16)


def heads_call(kernel, flags, tensors, outs, scratch, limit, flops):
    def spec(value):
        return pl.BlockSpec((value.shape[0], HEAD_DIM), lambda h: (0, h))

    out_specs = tuple(spec(out) for out in outs)
    return pl.pallas_call(
        kernel,
        grid=(tensors[0].shape[1] // HEAD_DIM,),
        in_specs=[pl.BlockSpec(memory_space=pltpu.SMEM)] + [spec(t) for t in tensors],
        out_specs=out_specs if len(outs) > 1 else out_specs[0],
        out_shape=tuple(outs) if len(outs) > 1 else outs[0],
        scratch_shapes=scratch,
        compiler_params=pltpu.CompilerParams(vmem_limit_bytes=limit * MIB),
        cost_estimate=pl.CostEstimate(flops=flops, bytes_accessed=6 * 10**6, transcendentals=0),
    )(flags, *tensors)


def in_hbm(values):
    return [pltpu.with_memory_space_constraint(value, pltpu.HBM) for value in values]


def attend_main(flags, tensors):
    rows, width = tensors[0].shape
    outs = [jax.ShapeDtypeStruct((rows, width), jnp.float32)] * 3
    scratch = [
        pltpu.VMEM((rows, KEYS), jnp.float32),
        pltpu.VMEM((rows, KEYS), jnp.bfloat16),
        pltpu.VMEM((KEYS, 2 * HEAD_DIM), jnp.bfloat16),
    ]
    return heads_call(main_kernel, flags, in_hbm(tensors), outs, scratch, 32, 3 * 10**9)


def attend_late(flags, tensors):
    rows, width = tensors[0].shape
    outs = [jax.ShapeDtypeStruct((rows, width), jnp.bfloat16)]
    scratch = [pltpu.VMEM((LATE, 2 * HEAD_DIM), jnp.bfloat16)]
    return heads_call(late_kernel, flags, tensors, outs, scratch, 16, 3 * 10**8)


def project_kernel(column, a_ref, b_ref, wa_ref, wb_ref, out_ref):
    total = dot(a_ref[...], wa_ref[...]) + dot(b_ref[...], wb_ref[...])
    out_ref[...] = total.astype(out_ref.dtype)


def project(column, own, peer, own_weight, peer_weight, dtype):
    rows, width = own.shape
    block = pl.BlockSpec((rows, width), lambda i, c: (0, 0))
    weight = pl.BlockSpec((width, width), lambda i, c: (0, c[0]))
    return pl.pallas_call(
        project_kernel,
        grid_spec=pltpu.PrefetchScalarGridSpec(
            num_scalar_prefetch=1,
            grid=(1,),
            in_specs=[block, block, weight, weight],
            out_specs=block,
        ),
        out_shape=jax.ShapeDtypeStruct((rows, width), dtype),
        compiler_params=pltpu.CompilerParams(vmem_limit_bytes=12 * MIB),
        cost_estimate=pl.CostEstimate(flops=10**9, bytes_accessed=10**6, transcendentals=0),
    )(column, own, peer, own_weight, peer_weight)


def layer(queries, key_rows, value_rows, out_weight):
    device = lax.axis_index("seq")
    head = lax.axis_index("head")
    last = lax.axis_size("seq") - 1
    lines = lax.axis_size("seq") // 4
    line = device // 4
    spot = device % 4
    even = line % 2 == 0

    raw, own_one, own_two = coarse(key_rows, value_rows)
    across = seq_permute(own_one, lambda i: i ^ 2)
    peer_weight = head_permute(out_weight, 1)
    two_half = small(half_kernel, own_two, across)
    two_beside = seq_permute(two_half, lambda i: i ^ 1)
    far = seq_permute(across, lambda i: i + 4 if i % 4 < 2 else i - 4)
    left = seq_permute(raw, lambda i: i + 1)
    right = seq_permute(raw, lambda i: i - 1)
    two_block, three_block = small(pack_kernel, two_half, two_beside, rows=(512, 256))
    two_low = seq_permute(two_block, lambda i: i + 4)
    two_high = seq_permute(two_block, lambda i: i - 4)
    outer = (spot == 0) | (spot == 3)
    handed = jnp.where(outer, far, across)
    third = seq_permute(handed, lambda i: i ^ 1)
    three_skew = seq_permute(three_block, lambda i: i + 12 if i // 4 % 2 == 0 else i - 12)
    near_low = small(halve_kernel, two_low)
    near_high = small(halve_kernel, two_high)
    three_low = seq_permute(near_low, lambda i: i + 4)
    three_high = seq_permute(near_high, lambda i: i - 4)

    far_ok = jnp.where(spot < 2, line > 0, line < lines - 1)
    flags = jnp.stack(
        [
            device > 0,
            device < last,
            spot % 2 == 0,
            line > 0,
            line < lines - 1,
            line >= 2,
            even,
            line < lines - 2,
            jnp.where(even, line < lines - 3, line >= 3),
            jnp.where(even, line > 0, line < lines - 1),
            far_ok,
            outer | far_ok,
            jnp.logical_not(outer) | far_ok,
        ]
    ).astype(jnp.int32)
    tensors = [queries, key_rows, value_rows, left, right, across, far, third]
    tensors += [two_low, two_high, three_skew, near_low, near_high]
    partial = attend_main(flags, tensors)
    attended = attend_late(flags, [queries, *partial, three_low, three_high])
    peer = head_permute(attended, 1)
    here_column, away_column = head.reshape(1), (head ^ 2).reshape(1)
    weights = (out_weight, peer_weight)
    away = project(away_column, attended, peer, *weights, jnp.bfloat16)
    arrived = head_permute(away, 2)
    here = project(here_column, attended, peer, *weights, jnp.float32)
    return (here + arrived.astype(jnp.float32)).astype(jnp.bfloat16)


def solution(mesh):
    in_specs = (P("seq", "head"), P("seq", "head"), P("seq", "head"), P("head", None))
    out_specs = P("seq", "head")
    return jax.shard_map(layer, mesh=mesh, in_specs=in_specs, out_specs=out_specs, check_vma=False)
```

```python
import jax
import jax.numpy as jnp
from jax import lax
from jax.experimental import pallas as pl
from jax.experimental.pallas import tpu as pltpu
from jax.sharding import PartitionSpec as P


HEAD_DIM = 128
LOG2E = 1.4426950408889634
MIB = 1024 * 1024


def seq_permute(value, target_of):
    count = lax.axis_size("seq")
    pairs = [(i, target_of(i)) for i in range(count)]
    pairs = [(i, j) for i, j in pairs if 0 <= j < count]
    return lax.ppermute(value, "seq", pairs)


def head_permute(value, bit):
    count = lax.axis_size("head")
    return lax.ppermute(value, "head", [(i, i ^ bit) for i in range(count)])


def mean_matrix(rows, factor):
    row = lax.broadcasted_iota(jnp.int32, (rows, rows * factor), 0)
    col = lax.broadcasted_iota(jnp.int32, (rows, rows * factor), 1)
    return jnp.where(col // factor == row, 1.0 / factor, 0.0).astype(jnp.bfloat16)


def spread_mean_matrix(rows, factor):
    row = lax.broadcasted_iota(jnp.int32, (rows, rows), 0)
    col = lax.broadcasted_iota(jnp.int32, (rows, rows), 1)
    return jnp.where(col // factor == row // factor, 1.0 / factor, 0.0).astype(jnp.bfloat16)


def dot(left, right):
    return jnp.dot(left, right, preferred_element_type=jnp.float32)


def dot_t(left, right):
    return lax.dot_general(left, right, (((1,), (1,)), ((), ())), preferred_element_type=jnp.float32)


def coarse_kernel(k_ref, v_ref, raw_ref, one_ref, two_ref, three_ref):
    half, quarter, eighth = mean_matrix(128, 2), mean_matrix(64, 4), mean_matrix(32, 8)
    for index, ref in enumerate((k_ref, v_ref)):
        value = ref[...]
        raw_ref[index * 256 : (index + 1) * 256] = value
        one_ref[index * 128 : (index + 1) * 128] = dot(half, value).astype(jnp.bfloat16)
        two_ref[index * 64 : (index + 1) * 64] = dot(quarter, value).astype(jnp.bfloat16)
        three_ref[index * 32 : (index + 1) * 32] = dot(eighth, value).astype(jnp.bfloat16)


def coarse(k, v):
    width = k.shape[1]
    return pl.pallas_call(
        coarse_kernel,
        out_shape=(
            jax.ShapeDtypeStruct((512, width), jnp.bfloat16),
            jax.ShapeDtypeStruct((256, width), jnp.bfloat16),
            jax.ShapeDtypeStruct((128, width), jnp.bfloat16),
            jax.ShapeDtypeStruct((64, width), jnp.bfloat16),
        ),
        compiler_params=pltpu.CompilerParams(vmem_limit_bytes=8 * MIB),
        cost_estimate=pl.CostEstimate(flops=10**8, bytes_accessed=10**6, transcendentals=0),
        name="coarse",
    )(k, v)


def half_kernel(two_ref, one_ref, out_ref):
    half = mean_matrix(64, 2)
    for part in range(2):
        base = part * 128
        out_ref[base : base + 64] = two_ref[part * 64 : (part + 1) * 64]
        out_ref[base + 64 : base + 128] = dot(half, one_ref[base : base + 128]).astype(jnp.bfloat16)


def halve_kernel(block_ref, out_ref):
    half = mean_matrix(128, 2)
    for part in range(2):
        out_ref[part * 128 : (part + 1) * 128] = dot(
            half, block_ref[part * 256 : (part + 1) * 256]
        ).astype(jnp.bfloat16)


def pack_kernel(a_ref, b_ref, out_ref):
    for part in range(2):
        for index, ref in enumerate((a_ref, b_ref)):
            start = part * 256 + index * 128
            out_ref[start : start + 128] = ref[part * 128 : (part + 1) * 128]


def hand_kernel(outer, far_ref, across_ref, skew_ref, skew_across_ref, out_ref):
    out_ref[:256] = jnp.where(outer[0] > 0, far_ref[...], across_ref[...])
    out_ref[256:320] = skew_ref[...]
    out_ref[320:384] = skew_across_ref[...]


def hand(outer, far, across, skew, skew_across):
    whole = pl.BlockSpec(memory_space=pltpu.VMEM)
    return pl.pallas_call(
        hand_kernel,
        in_specs=[pl.BlockSpec(memory_space=pltpu.SMEM)] + [whole] * 4,
        out_specs=whole,
        out_shape=jax.ShapeDtypeStruct((384, far.shape[1]), far.dtype),
        compiler_params=pltpu.CompilerParams(vmem_limit_bytes=4 * MIB),
        cost_estimate=pl.CostEstimate(flops=10**8, bytes_accessed=10**6, transcendentals=0),
        name="hand",
    )(outer, far, across, skew, skew_across)


def small(kernel, *operands, rows=(256,)):
    width, dtype = operands[0].shape[1], operands[0].dtype
    shapes = tuple(jax.ShapeDtypeStruct((count, width), dtype) for count in rows)
    return pl.pallas_call(
        kernel,
        out_shape=shapes if len(rows) > 1 else shapes[0],
        compiler_params=pltpu.CompilerParams(vmem_limit_bytes=4 * MIB),
        cost_estimate=pl.CostEstimate(flops=10**8, bytes_accessed=10**6, transcendentals=0),
    )(*operands)


LATE = 2 * 128
KEYS = 768 + 3 * 512 - LATE
SCALE = LOG2E * HEAD_DIM**-0.5


def bias(flags, index):
    return jnp.where(flags[index] > 0, 0.0, -jnp.inf)


def main_kernel(flags, q_ref, *refs):
    k_ref, v_ref, left, right = refs[0:4]
    across, far, third = refs[4:7]
    twos = refs[7:9]
    skews = refs[9:11]
    nears = refs[11:13]
    sum_ref, weight_ref, top_ref = refs[13:16]
    scores, weights, values = refs[16:19]

    rows = q_ref.shape[0]
    even = flags[6] > 0
    beside_left = flags[2] > 0
    half = mean_matrix(128, 2)
    spreads = [spread_mean_matrix(rows, 2**level) for level in range(1, 4)]
    for slot in range(2):
        values[slot, :, HEAD_DIM:] = jnp.ones((KEYS, HEAD_DIM), jnp.bfloat16)

    for head in range(q_ref.shape[1] // HEAD_DIM):
        slot = head % 2
        lanes = slice(head * HEAD_DIM, (head + 1) * HEAD_DIM)

        def rows_of(ref, start, count):
            return ref[start : start + count, lanes]

        def either(flag, first, second, start, count):
            return jnp.where(flag, rows_of(first, start, count), rows_of(second, start, count))

        fourth = [
            dot(half, either(beside_left, left, right, part * 256, 256)).astype(jnp.bfloat16)
            for part in range(2)
        ]
        near = [either(even, nears[0], nears[1], part * 128, 128) for part in range(2)]
        skew = [
            jnp.concatenate(
                [
                    rows_of(skews[0], part * 32, 32),
                    rows_of(skews[1], part * 32, 32),
                    rows_of(third, 256 + part * 32, 32),
                    rows_of(third, 320 + part * 32, 32),
                ],
                0,
            )
            for part in range(2)
        ]
        pieces = [(rows_of(k_ref, 0, 256), rows_of(v_ref, 0, 256), 0, None)]
        for index, ref in enumerate((left, right)):
            pieces.append((rows_of(ref, 0, 256), rows_of(ref, 256, 256), 0, index))
        for ref, flag in ((across, None), (far, 10), (third, 11)):
            pieces.append((rows_of(ref, 0, 128), rows_of(ref, 128, 128), 1, flag))
        pieces.append((fourth[0], fourth[1], 1, 12))
        for index, ref in enumerate(twos):
            pieces.append((rows_of(ref, 0, 256), rows_of(ref, 256, 256), 2, 3 + index))
        pieces.append((skew[0], skew[1], 3, 8))
        pieces.append((near[0], near[1], 3, 9))

        query = rows_of(q_ref, 0, rows)
        queries = [query] + [dot(spread, query).astype(jnp.bfloat16) for spread in spreads]
        largest = None
        start = 0
        spans = []
        for keys, vals, level, flag in pieces:
            count = keys.shape[0]
            part = dot_t(queries[level], keys)
            if flag is not None:
                part = part + bias(flags, flag)
            scores[slot, :, start : start + count] = part
            values[slot, start : start + count, :HEAD_DIM] = vals
            for column in range(0, count, 128):
                piece = part[:, column : column + 128]
                largest = piece if largest is None else jnp.maximum(largest, piece)
            spans.append((start, count, level))
            start += count
        top = jnp.max(largest, axis=1, keepdims=True) * SCALE
        for start, count, level in spans:
            shifted = scores[slot, :, start : start + count] * SCALE - (top - level)
            weights[slot, :, start : start + count] = jnp.exp2(shifted).astype(jnp.bfloat16)
        total = dot(weights[slot], values[slot])
        sum_ref[:, lanes] = total[:, :HEAD_DIM]
        weight_ref[:, lanes] = total[:, HEAD_DIM:]
        top_ref[:, lanes] = jnp.broadcast_to(top, (rows, HEAD_DIM))


def late_kernel(flags, q_ref, sum_ref, weight_ref, top_ref, low, high, out_ref, values):
    rows = q_ref.shape[0]
    spread = spread_mean_matrix(rows, 8)
    for slot in range(2):
        values[slot, :, HEAD_DIM:] = jnp.ones((LATE, HEAD_DIM), jnp.bfloat16)
    for head in range(q_ref.shape[1] // HEAD_DIM):
        slot = head % 2
        lanes = slice(head * HEAD_DIM, (head + 1) * HEAD_DIM)
        query = dot(spread, q_ref[:, lanes]).astype(jnp.bfloat16)
        parts = []
        for index, (ref, flag) in enumerate(((low, 5), (high, 7))):
            parts.append(dot_t(query, ref[:128, lanes]) + bias(flags, flag))
            values[slot, index * 128 : (index + 1) * 128, :HEAD_DIM] = ref[128:, lanes]
        early = top_ref[:, lanes]
        top = jnp.max(jnp.maximum(parts[0], parts[1]), axis=1, keepdims=True) * SCALE
        top = jnp.maximum(early, top)
        kept = jnp.exp2(early - top)
        part = jnp.concatenate([jnp.exp2(p * SCALE - (top - 3.0)) for p in parts], 1)
        total = dot(part.astype(jnp.bfloat16), values[slot])
        numerator = sum_ref[:, lanes] * kept + total[:, :HEAD_DIM]
        denominator = weight_ref[:, lanes] * kept + total[:, HEAD_DIM:]
        out_ref[:, lanes] = (numerator / denominator).astype(jnp.bfloat16)


def heads_call(kernel, flags, tensors, outs, scratch, limit, flops):
    whole = pl.BlockSpec(memory_space=pltpu.VMEM)
    several = len(outs) > 1
    return pl.pallas_call(
        kernel,
        in_specs=[pl.BlockSpec(memory_space=pltpu.SMEM)] + [whole] * len(tensors),
        out_specs=(whole,) * len(outs) if several else whole,
        out_shape=tuple(outs) if several else outs[0],
        scratch_shapes=scratch,
        compiler_params=pltpu.CompilerParams(vmem_limit_bytes=limit * MIB),
        cost_estimate=pl.CostEstimate(flops=flops, bytes_accessed=6 * 10**6, transcendentals=0),
    )(flags, *tensors)


def attend_main(flags, tensors):
    rows, width = tensors[0].shape
    outs = [jax.ShapeDtypeStruct((rows, width), jnp.float32)] * 3
    scratch = [
        pltpu.VMEM((2, rows, KEYS), jnp.float32),
        pltpu.VMEM((2, rows, KEYS), jnp.bfloat16),
        pltpu.VMEM((2, KEYS, 2 * HEAD_DIM), jnp.bfloat16),
    ]
    return heads_call(main_kernel, flags, tensors, outs, scratch, 32, 3 * 10**9)


def attend_late(flags, tensors):
    rows, width = tensors[0].shape
    outs = [jax.ShapeDtypeStruct((rows, width), jnp.bfloat16)]
    scratch = [pltpu.VMEM((2, LATE, 2 * HEAD_DIM), jnp.bfloat16)]
    return heads_call(late_kernel, flags, tensors, outs, scratch, 16, 3 * 10**8)


def project_kernel(column, a_ref, b_ref, wa_ref, wb_ref, out_ref):
    total = dot(a_ref[...], wa_ref[...]) + dot(b_ref[...], wb_ref[...])
    out_ref[...] = total.astype(out_ref.dtype)


def project(column, own, peer, own_weight, peer_weight, dtype):
    rows, width = own.shape
    block = pl.BlockSpec((rows, width), lambda i, c: (0, 0))
    weight = pl.BlockSpec((width, width), lambda i, c: (0, c[0]))
    return pl.pallas_call(
        project_kernel,
        grid_spec=pltpu.PrefetchScalarGridSpec(
            num_scalar_prefetch=1,
            grid=(1,),
            in_specs=[block, block, weight, weight],
            out_specs=block,
        ),
        out_shape=jax.ShapeDtypeStruct((rows, width), dtype),
        compiler_params=pltpu.CompilerParams(vmem_limit_bytes=12 * MIB),
        cost_estimate=pl.CostEstimate(flops=10**9, bytes_accessed=10**6, transcendentals=0),
    )(column, own, peer, own_weight, peer_weight)


def layer(queries, key_rows, value_rows, out_weight):
    device = lax.axis_index("seq")
    head = lax.axis_index("head")
    last = lax.axis_size("seq") - 1
    lines = lax.axis_size("seq") // 4
    line = device // 4
    spot = device % 4
    even = line % 2 == 0

    raw, own_one, own_two, own_three = coarse(key_rows, value_rows)
    across = seq_permute(own_one, lambda i: i ^ 2)
    skew = seq_permute(own_three, lambda i: i + 12 if i // 4 % 2 == 0 else i - 12)
    peer_weight = head_permute(out_weight, 1)
    two_half = small(half_kernel, own_two, across)
    two_beside = seq_permute(two_half, lambda i: i ^ 1)
    skew_across = seq_permute(skew, lambda i: i ^ 2)
    far = seq_permute(across, lambda i: i + 4 if i % 4 < 2 else i - 4)
    left = seq_permute(raw, lambda i: i + 1)
    right = seq_permute(raw, lambda i: i - 1)
    two_block = small(pack_kernel, two_half, two_beside, rows=(512,))
    two_low = seq_permute(two_block, lambda i: i + 4)
    two_high = seq_permute(two_block, lambda i: i - 4)
    outer = (spot == 0) | (spot == 3)
    handed = hand(outer.astype(jnp.int32).reshape(1), far, across, skew, skew_across)
    third = seq_permute(handed, lambda i: i ^ 1)
    near_low = small(halve_kernel, two_low)
    near_high = small(halve_kernel, two_high)
    three_low = seq_permute(near_low, lambda i: i + 4)
    three_high = seq_permute(near_high, lambda i: i - 4)

    far_ok = jnp.where(spot < 2, line > 0, line < lines - 1)
    flags = jnp.stack(
        [
            device > 0,
            device < last,
            spot % 2 == 0,
            line > 0,
            line < lines - 1,
            line >= 2,
            even,
            line < lines - 2,
            jnp.where(even, line < lines - 3, line >= 3),
            jnp.where(even, line > 0, line < lines - 1),
            far_ok,
            outer | far_ok,
            jnp.logical_not(outer) | far_ok,
        ]
    ).astype(jnp.int32)
    tensors = [queries, key_rows, value_rows, left, right, across, far, third]
    tensors += [two_low, two_high, skew, skew_across, near_low, near_high]
    partial = attend_main(flags, tensors)
    attended = attend_late(flags, [queries, *partial, three_low, three_high])
    peer = head_permute(attended, 1)
    here_column, away_column = head.reshape(1), (head ^ 2).reshape(1)
    weights = (out_weight, peer_weight)
    away = project(away_column, attended, peer, *weights, jnp.bfloat16)
    arrived = head_permute(away, 2)
    here = project(here_column, attended, peer, *weights, jnp.float32)
    return (here + arrived.astype(jnp.float32)).astype(jnp.bfloat16)


def solution(mesh):
    in_specs = (P("seq", "head"), P("seq", "head"), P("seq", "head"), P("head", None))
    out_specs = P("seq", "head")
    return jax.shard_map(layer, mesh=mesh, in_specs=in_specs, out_specs=out_specs, check_vma=False)
```

```python
import jax
import jax.numpy as jnp
from jax import lax
from jax.experimental import pallas as pl
from jax.experimental.pallas import tpu as pltpu
from jax.sharding import PartitionSpec as P


HEAD_DIM = 128
LOG2E = 1.4426950408889634
MIB = 1024 * 1024


def in_hbm(values):
    return [pltpu.with_memory_space_constraint(value, pltpu.HBM) for value in values]


def seq_permute(value, target_of):
    count = lax.axis_size("seq")
    pairs = [(i, target_of(i)) for i in range(count)]
    pairs = [(i, j) for i, j in pairs if 0 <= j < count]
    return lax.ppermute(value, "seq", pairs)


def head_permute(value, bit):
    count = lax.axis_size("head")
    return lax.ppermute(value, "head", [(i, i ^ bit) for i in range(count)])


def mean_matrix(rows, factor):
    row = lax.broadcasted_iota(jnp.int32, (rows, rows * factor), 0)
    col = lax.broadcasted_iota(jnp.int32, (rows, rows * factor), 1)
    return jnp.where(col // factor == row, 1.0 / factor, 0.0).astype(jnp.bfloat16)


def spread_mean_matrix(rows, factor):
    row = lax.broadcasted_iota(jnp.int32, (rows, rows), 0)
    col = lax.broadcasted_iota(jnp.int32, (rows, rows), 1)
    return jnp.where(col // factor == row // factor, 1.0 / factor, 0.0).astype(jnp.bfloat16)


def dot(left, right):
    return jnp.dot(left, right, preferred_element_type=jnp.float32)


def dot_t(left, right):
    return lax.dot_general(left, right, (((1,), (1,)), ((), ())), preferred_element_type=jnp.float32)


def coarse_kernel(k_ref, v_ref, raw_ref, one_ref, two_ref, three_ref):
    half, quarter, eighth = mean_matrix(128, 2), mean_matrix(64, 4), mean_matrix(32, 8)
    for index, ref in enumerate((k_ref, v_ref)):
        value = ref[...]
        raw_ref[index * 256 : (index + 1) * 256] = value
        one_ref[index * 128 : (index + 1) * 128] = dot(half, value).astype(jnp.bfloat16)
        two_ref[index * 64 : (index + 1) * 64] = dot(quarter, value).astype(jnp.bfloat16)
        three_ref[index * 32 : (index + 1) * 32] = dot(eighth, value).astype(jnp.bfloat16)


def coarse(k, v):
    width = k.shape[1]
    return pl.pallas_call(
        coarse_kernel,
        out_shape=(
            jax.ShapeDtypeStruct((512, width), jnp.bfloat16),
            jax.ShapeDtypeStruct((256, width), jnp.bfloat16),
            jax.ShapeDtypeStruct((128, width), jnp.bfloat16),
            jax.ShapeDtypeStruct((64, width), jnp.bfloat16),
        ),
        compiler_params=pltpu.CompilerParams(vmem_limit_bytes=8 * MIB),
        cost_estimate=pl.CostEstimate(flops=10**8, bytes_accessed=10**6, transcendentals=0),
        name="coarse",
    )(*in_hbm((k, v)))


def half_kernel(two_ref, one_ref, out_ref):
    half = mean_matrix(64, 2)
    for part in range(2):
        base = part * 128
        out_ref[base : base + 64] = two_ref[part * 64 : (part + 1) * 64]
        out_ref[base + 64 : base + 128] = dot(half, one_ref[base : base + 128]).astype(jnp.bfloat16)


def halve_kernel(block_ref, out_ref):
    half = mean_matrix(128, 2)
    for part in range(2):
        out_ref[part * 128 : (part + 1) * 128] = dot(
            half, block_ref[part * 256 : (part + 1) * 256]
        ).astype(jnp.bfloat16)


def pack_kernel(a_ref, b_ref, out_ref):
    for part in range(2):
        for index, ref in enumerate((a_ref, b_ref)):
            start = part * 256 + index * 128
            out_ref[start : start + 128] = ref[part * 128 : (part + 1) * 128]


def hand_kernel(outer, far_ref, across_ref, skew_ref, skew_across_ref, out_ref):
    out_ref[:256] = jnp.where(outer[0] > 0, far_ref[...], across_ref[...])
    out_ref[256:320] = skew_ref[...]
    out_ref[320:384] = skew_across_ref[...]


def hand(outer, far, across, skew, skew_across):
    whole = pl.BlockSpec(memory_space=pltpu.VMEM)
    return pl.pallas_call(
        hand_kernel,
        in_specs=[pl.BlockSpec(memory_space=pltpu.SMEM)] + [whole] * 4,
        out_specs=whole,
        out_shape=jax.ShapeDtypeStruct((384, far.shape[1]), far.dtype),
        compiler_params=pltpu.CompilerParams(vmem_limit_bytes=4 * MIB),
        cost_estimate=pl.CostEstimate(flops=10**8, bytes_accessed=10**6, transcendentals=0),
        name="hand",
    )(outer, far, across, skew, skew_across)


def small(kernel, *operands, rows=(256,)):
    width, dtype = operands[0].shape[1], operands[0].dtype
    shapes = tuple(jax.ShapeDtypeStruct((count, width), dtype) for count in rows)
    return pl.pallas_call(
        kernel,
        out_shape=shapes if len(rows) > 1 else shapes[0],
        compiler_params=pltpu.CompilerParams(vmem_limit_bytes=4 * MIB),
        cost_estimate=pl.CostEstimate(flops=10**8, bytes_accessed=10**6, transcendentals=0),
    )(*operands)


LATE = 2 * 128
KEYS = 768 + 3 * 512 - LATE
SCALE = LOG2E * HEAD_DIM**-0.5


def bias(flags, index):
    return jnp.where(flags[index] > 0, 0.0, -jnp.inf)


def main_kernel(flags, q_ref, *refs):
    k_ref, v_ref = refs[0:2]
    across, far = refs[4:6]
    twos = refs[7:9]
    skews = refs[9:11]
    nears = refs[11:13]
    sum_ref, weight_ref, top_ref = refs[13:16]
    scores, weights, values, left, right, third, arrived = refs[16:23]
    copies = [
        pltpu.make_async_copy(source, target, arrived.at[index])
        for index, (source, target) in enumerate(
            ((refs[2], left), (refs[3], right), (refs[6], third))
        )
    ]
    for copy in copies:
        copy.start()

    rows = q_ref.shape[0]
    even = flags[6] > 0
    beside_left = flags[2] > 0
    half = mean_matrix(128, 2)
    spreads = [spread_mean_matrix(rows, 2**level) for level in range(1, 4)]
    for slot in range(2):
        values[slot, :, HEAD_DIM:] = jnp.ones((KEYS, HEAD_DIM), jnp.bfloat16)

    for head in range(q_ref.shape[1] // HEAD_DIM):
        slot = head % 2
        lanes = slice(head * HEAD_DIM, (head + 1) * HEAD_DIM)

        def rows_of(ref, start, count):
            return ref[start : start + count, lanes]

        def either(flag, first, second, start, count):
            return jnp.where(flag, rows_of(first, start, count), rows_of(second, start, count))

        query = rows_of(q_ref, 0, rows)
        queries = [query] + [dot(spread, query).astype(jnp.bfloat16) for spread in spreads]
        largest = None
        spans = []

        def take(keys, vals, level, flag):
            nonlocal largest
            start = spans[-1][0] + spans[-1][1] if spans else 0
            count = keys.shape[0]
            part = dot_t(queries[level], keys)
            if flag is not None:
                part = part + bias(flags, flag)
            scores[slot, :, start : start + count] = part
            values[slot, start : start + count, :HEAD_DIM] = vals
            for column in range(0, count, 128):
                piece = part[:, column : column + 128]
                largest = piece if largest is None else jnp.maximum(largest, piece)
            spans.append((start, count, level))

        take(rows_of(k_ref, 0, 256), rows_of(v_ref, 0, 256), 0, None)
        for index, ref in enumerate(twos):
            take(rows_of(ref, 0, 256), rows_of(ref, 256, 256), 2, 3 + index)
        near = [either(even, nears[0], nears[1], part * 128, 128) for part in range(2)]
        take(near[0], near[1], 3, 9)
        for ref, flag in ((across, None), (far, 10)):
            take(rows_of(ref, 0, 128), rows_of(ref, 128, 128), 1, flag)
        if head == 0:
            for copy in copies:
                copy.wait()
        take(rows_of(third, 0, 128), rows_of(third, 128, 128), 1, 11)
        skew = [
            jnp.concatenate(
                [
                    rows_of(skews[0], part * 32, 32),
                    rows_of(skews[1], part * 32, 32),
                    rows_of(third, 256 + part * 32, 32),
                    rows_of(third, 320 + part * 32, 32),
                ],
                0,
            )
            for part in range(2)
        ]
        take(skew[0], skew[1], 3, 8)
        for index, ref in enumerate((left, right)):
            take(rows_of(ref, 0, 256), rows_of(ref, 256, 256), 0, index)
        fourth = [
            dot(half, either(beside_left, left, right, part * 256, 256)).astype(jnp.bfloat16)
            for part in range(2)
        ]
        take(fourth[0], fourth[1], 1, 12)
        top = jnp.max(largest, axis=1, keepdims=True) * SCALE
        for start, count, level in spans:
            shifted = scores[slot, :, start : start + count] * SCALE - (top - level)
            weights[slot, :, start : start + count] = jnp.exp2(shifted).astype(jnp.bfloat16)
        total = dot(weights[slot], values[slot])
        sum_ref[:, lanes] = total[:, :HEAD_DIM]
        weight_ref[:, lanes] = total[:, HEAD_DIM:]
        top_ref[:, lanes] = jnp.broadcast_to(top, (rows, HEAD_DIM))


def late_kernel(flags, q_ref, sum_ref, weight_ref, top_ref, low, high, out_ref, values):
    rows = q_ref.shape[0]
    spread = spread_mean_matrix(rows, 8)
    for slot in range(2):
        values[slot, :, HEAD_DIM:] = jnp.ones((LATE, HEAD_DIM), jnp.bfloat16)
    for head in range(q_ref.shape[1] // HEAD_DIM):
        slot = head % 2
        lanes = slice(head * HEAD_DIM, (head + 1) * HEAD_DIM)
        query = dot(spread, q_ref[:, lanes]).astype(jnp.bfloat16)
        parts = []
        for index, (ref, flag) in enumerate(((low, 5), (high, 7))):
            parts.append(dot_t(query, ref[:128, lanes]) + bias(flags, flag))
            values[slot, index * 128 : (index + 1) * 128, :HEAD_DIM] = ref[128:, lanes]
        early = top_ref[:, lanes]
        top = jnp.max(jnp.maximum(parts[0], parts[1]), axis=1, keepdims=True) * SCALE
        top = jnp.maximum(early, top)
        kept = jnp.exp2(early - top)
        part = jnp.concatenate([jnp.exp2(p * SCALE - (top - 3.0)) for p in parts], 1)
        total = dot(part.astype(jnp.bfloat16), values[slot])
        numerator = sum_ref[:, lanes] * kept + total[:, :HEAD_DIM]
        denominator = weight_ref[:, lanes] * kept + total[:, HEAD_DIM:]
        out_ref[:, lanes] = (numerator / denominator).astype(jnp.bfloat16)


def heads_call(kernel, flags, tensors, outs, scratch, limit, flops, away=()):
    whole = pl.BlockSpec(memory_space=pltpu.VMEM)
    several = len(outs) > 1
    return pl.pallas_call(
        kernel,
        in_specs=[pl.BlockSpec(memory_space=pltpu.SMEM)]
        + [pl.BlockSpec(memory_space=pl.ANY) if i in away else whole for i in range(len(tensors))],
        out_specs=(whole,) * len(outs) if several else whole,
        out_shape=tuple(outs) if several else outs[0],
        scratch_shapes=scratch,
        compiler_params=pltpu.CompilerParams(vmem_limit_bytes=limit * MIB),
        cost_estimate=pl.CostEstimate(flops=flops, bytes_accessed=6 * 10**6, transcendentals=0),
    )(flags, *tensors)


def attend_main(flags, tensors):
    rows, width = tensors[0].shape
    outs = [jax.ShapeDtypeStruct((rows, width), jnp.float32)] * 3
    scratch = [
        pltpu.VMEM((2, rows, KEYS), jnp.float32),
        pltpu.VMEM((2, rows, KEYS), jnp.bfloat16),
        pltpu.VMEM((2, KEYS, 2 * HEAD_DIM), jnp.bfloat16),
    ]
    away = (3, 4, 7)
    scratch += [pltpu.VMEM(tensors[i].shape, jnp.bfloat16) for i in away]
    scratch.append(pltpu.SemaphoreType.DMA((len(away),)))
    return heads_call(main_kernel, flags, tensors, outs, scratch, 32, 3 * 10**9, away)


def attend_late(flags, tensors):
    rows, width = tensors[0].shape
    outs = [jax.ShapeDtypeStruct((rows, width), jnp.bfloat16)]
    scratch = [pltpu.VMEM((2, LATE, 2 * HEAD_DIM), jnp.bfloat16)]
    return heads_call(late_kernel, flags, tensors, outs, scratch, 16, 3 * 10**8)


def project_kernel(column, a_ref, b_ref, wa_ref, wb_ref, out_ref):
    total = dot(a_ref[...], wa_ref[...]) + dot(b_ref[...], wb_ref[...])
    out_ref[...] = total.astype(out_ref.dtype)


def project(column, own, peer, own_weight, peer_weight, dtype):
    rows, width = own.shape
    block = pl.BlockSpec((rows, width), lambda i, c: (0, 0))
    weight = pl.BlockSpec((width, width), lambda i, c: (0, c[0]))
    return pl.pallas_call(
        project_kernel,
        grid_spec=pltpu.PrefetchScalarGridSpec(
            num_scalar_prefetch=1,
            grid=(1,),
            in_specs=[block, block, weight, weight],
            out_specs=block,
        ),
        out_shape=jax.ShapeDtypeStruct((rows, width), dtype),
        compiler_params=pltpu.CompilerParams(vmem_limit_bytes=12 * MIB),
        cost_estimate=pl.CostEstimate(flops=10**9, bytes_accessed=10**6, transcendentals=0),
    )(column, own, peer, own_weight, peer_weight)


def layer(queries, key_rows, value_rows, out_weight):
    device = lax.axis_index("seq")
    head = lax.axis_index("head")
    last = lax.axis_size("seq") - 1
    lines = lax.axis_size("seq") // 4
    line = device // 4
    spot = device % 4
    even = line % 2 == 0

    raw, own_one, own_two, own_three = coarse(key_rows, value_rows)
    across = seq_permute(own_one, lambda i: i ^ 2)
    skew = seq_permute(own_three, lambda i: i + 12 if i // 4 % 2 == 0 else i - 12)
    peer_weight = head_permute(out_weight, 1)
    two_half = small(half_kernel, own_two, across)
    two_beside = seq_permute(two_half, lambda i: i ^ 1)
    skew_across = seq_permute(skew, lambda i: i ^ 2)
    far = seq_permute(across, lambda i: i + 4 if i % 4 < 2 else i - 4)
    left = seq_permute(raw, lambda i: i + 1)
    right = seq_permute(raw, lambda i: i - 1)
    two_block = small(pack_kernel, two_half, two_beside, rows=(512,))
    two_low = seq_permute(two_block, lambda i: i + 4)
    two_high = seq_permute(two_block, lambda i: i - 4)
    outer = (spot == 0) | (spot == 3)
    handed = hand(outer.astype(jnp.int32).reshape(1), far, across, skew, skew_across)
    third = seq_permute(handed, lambda i: i ^ 1)
    near_low = small(halve_kernel, two_low)
    near_high = small(halve_kernel, two_high)
    three_low = seq_permute(near_low, lambda i: i + 4)
    three_high = seq_permute(near_high, lambda i: i - 4)

    far_ok = jnp.where(spot < 2, line > 0, line < lines - 1)
    flags = jnp.stack(
        [
            device > 0,
            device < last,
            spot % 2 == 0,
            line > 0,
            line < lines - 1,
            line >= 2,
            even,
            line < lines - 2,
            jnp.where(even, line < lines - 3, line >= 3),
            jnp.where(even, line > 0, line < lines - 1),
            far_ok,
            outer | far_ok,
            jnp.logical_not(outer) | far_ok,
        ]
    ).astype(jnp.int32)
    tensors = [queries, key_rows, value_rows, left, right, across, far, third]
    tensors += [two_low, two_high, skew, skew_across, near_low, near_high]
    partial = attend_main(flags, tensors)
    attended = attend_late(flags, [queries, *partial, three_low, three_high])
    peer = head_permute(attended, 1)
    here_column, away_column = head.reshape(1), (head ^ 2).reshape(1)
    weights = (out_weight, peer_weight)
    away = project(away_column, attended, peer, *weights, jnp.bfloat16)
    arrived = head_permute(away, 2)
    here = project(here_column, attended, peer, *weights, jnp.float32)
    return (here + arrived.astype(jnp.float32)).astype(jnp.bfloat16)


def solution(mesh):
    in_specs = (P("seq", "head"), P("seq", "head"), P("seq", "head"), P("head", None))
    out_specs = P("seq", "head")
    return jax.shard_map(layer, mesh=mesh, in_specs=in_specs, out_specs=out_specs, check_vma=False)
```

```python
import jax
import jax.numpy as jnp
from jax import lax
from jax.experimental import pallas as pl
from jax.experimental.pallas import tpu as pltpu
from jax.sharding import PartitionSpec as P


HEAD_DIM = 128
LOG2E = 1.4426950408889634
MIB = 1024 * 1024


def in_hbm(values):
    return [pltpu.with_memory_space_constraint(value, pltpu.HBM) for value in values]


def seq_permute(value, target_of):
    count = lax.axis_size("seq")
    pairs = [(i, target_of(i)) for i in range(count)]
    pairs = [(i, j) for i, j in pairs if 0 <= j < count]
    return lax.ppermute(value, "seq", pairs)


def head_permute(value, bit):
    count = lax.axis_size("head")
    return lax.ppermute(value, "head", [(i, i ^ bit) for i in range(count)])


def mean_matrix(rows, factor):
    row = lax.broadcasted_iota(jnp.int32, (rows, rows * factor), 0)
    col = lax.broadcasted_iota(jnp.int32, (rows, rows * factor), 1)
    return jnp.where(col // factor == row, 1.0 / factor, 0.0).astype(jnp.bfloat16)


def spread_mean_matrix(rows, factor):
    row = lax.broadcasted_iota(jnp.int32, (rows, rows), 0)
    col = lax.broadcasted_iota(jnp.int32, (rows, rows), 1)
    return jnp.where(col // factor == row // factor, 1.0 / factor, 0.0).astype(jnp.bfloat16)


def dot(left, right):
    return jnp.dot(left, right, preferred_element_type=jnp.float32)


def dot_t(left, right):
    return lax.dot_general(left, right, (((1,), (1,)), ((), ())), preferred_element_type=jnp.float32)


def coarse_kernel(k_ref, v_ref, raw_ref, one_ref, two_ref, three_ref):
    half, quarter, eighth = mean_matrix(128, 2), mean_matrix(64, 4), mean_matrix(32, 8)
    for index, ref in enumerate((k_ref, v_ref)):
        value = ref[...]
        raw_ref[index * 256 : (index + 1) * 256] = value
        one_ref[index * 128 : (index + 1) * 128] = dot(half, value).astype(jnp.bfloat16)
        two_ref[index * 64 : (index + 1) * 64] = dot(quarter, value).astype(jnp.bfloat16)
        three_ref[index * 32 : (index + 1) * 32] = dot(eighth, value).astype(jnp.bfloat16)


def coarse(k, v):
    width = k.shape[1]
    return pl.pallas_call(
        coarse_kernel,
        out_shape=(
            jax.ShapeDtypeStruct((512, width), jnp.bfloat16),
            jax.ShapeDtypeStruct((256, width), jnp.bfloat16),
            jax.ShapeDtypeStruct((128, width), jnp.bfloat16),
            jax.ShapeDtypeStruct((64, width), jnp.bfloat16),
        ),
        compiler_params=pltpu.CompilerParams(vmem_limit_bytes=8 * MIB),
        cost_estimate=pl.CostEstimate(flops=10**8, bytes_accessed=10**6, transcendentals=0),
        name="coarse",
    )(*in_hbm((k, v)))


def half_kernel(two_ref, one_ref, out_ref):
    half = mean_matrix(64, 2)
    for part in range(2):
        base = part * 128
        out_ref[base : base + 64] = two_ref[part * 64 : (part + 1) * 64]
        out_ref[base + 64 : base + 128] = dot(half, one_ref[base : base + 128]).astype(jnp.bfloat16)


def halve_kernel(block_ref, out_ref):
    half = mean_matrix(128, 2)
    for part in range(2):
        out_ref[part * 128 : (part + 1) * 128] = dot(
            half, block_ref[part * 256 : (part + 1) * 256]
        ).astype(jnp.bfloat16)


def pack_kernel(a_ref, b_ref, out_ref):
    for part in range(2):
        for index, ref in enumerate((a_ref, b_ref)):
            start = part * 256 + index * 128
            out_ref[start : start + 128] = ref[part * 128 : (part + 1) * 128]


def hand_kernel(outer, far_ref, across_ref, skew_ref, skew_across_ref, out_ref):
    out_ref[:256] = jnp.where(outer[0] > 0, far_ref[...], across_ref[...])
    out_ref[256:320] = skew_ref[...]
    out_ref[320:384] = skew_across_ref[...]


def hand(outer, far, across, skew, skew_across):
    whole = pl.BlockSpec(memory_space=pltpu.VMEM)
    return pl.pallas_call(
        hand_kernel,
        in_specs=[pl.BlockSpec(memory_space=pltpu.SMEM)] + [whole] * 4,
        out_specs=whole,
        out_shape=jax.ShapeDtypeStruct((384, far.shape[1]), far.dtype),
        compiler_params=pltpu.CompilerParams(vmem_limit_bytes=4 * MIB),
        cost_estimate=pl.CostEstimate(flops=10**8, bytes_accessed=10**6, transcendentals=0),
        name="hand",
    )(outer, far, across, skew, skew_across)


def small(kernel, *operands, rows=(256,)):
    width, dtype = operands[0].shape[1], operands[0].dtype
    shapes = tuple(jax.ShapeDtypeStruct((count, width), dtype) for count in rows)
    return pl.pallas_call(
        kernel,
        out_shape=shapes if len(rows) > 1 else shapes[0],
        compiler_params=pltpu.CompilerParams(vmem_limit_bytes=4 * MIB),
        cost_estimate=pl.CostEstimate(flops=10**8, bytes_accessed=10**6, transcendentals=0),
    )(*operands)


KEYS = 1152
SCALE = LOG2E * HEAD_DIM**-0.5


def bias(flags, index):
    return jnp.where(flags[index] > 0, 0.0, -jnp.inf)


class Pass:
    def __init__(self, slot, queries, flags, scores, weights, values):
        self.slot, self.queries, self.flags = slot, queries, flags
        self.scores, self.weights, self.values = scores, weights, values
        self.largest, self.spans = None, []

    def take(self, keys, vals, level, flag):
        start = self.spans[-1][0] + self.spans[-1][1] if self.spans else 0
        count = keys.shape[0]
        part = dot_t(self.queries[level], keys)
        if flag is not None:
            part = part + bias(self.flags, flag)
        self.scores[self.slot, :, start : start + count] = part
        self.values[self.slot, start : start + count, :HEAD_DIM] = vals
        for column in range(0, count, 128):
            piece = part[:, column : column + 128]
            self.largest = piece if self.largest is None else jnp.maximum(self.largest, piece)
        self.spans.append((start, count, level))

    def top(self):
        return jnp.max(self.largest, axis=1, keepdims=True) * SCALE

    def sums(self, top):
        for start, count, level in self.spans:
            shifted = self.scores[self.slot, :, start : start + count] * SCALE - (top - level)
            self.weights[self.slot, :, start : start + count] = jnp.exp2(shifted).astype(
                jnp.bfloat16
            )
        total = dot(self.weights[self.slot], self.values[self.slot])
        return total[:, :HEAD_DIM], total[:, HEAD_DIM:]


def start_head(head, q_ref, spreads, flags, scratch):
    lanes = slice(head * HEAD_DIM, (head + 1) * HEAD_DIM)
    query = q_ref[:, lanes]
    queries = {level: dot(spread, query).astype(jnp.bfloat16) for level, spread in spreads.items()}
    queries[0] = query
    return lanes, Pass(head % 2, queries, flags, *scratch)


def spreads_for(rows, levels, values):
    for slot in range(2):
        values[slot, :, HEAD_DIM:] = jnp.ones((KEYS, HEAD_DIM), jnp.bfloat16)
    return {level: spread_mean_matrix(rows, 2**level) for level in levels}


def main_kernel(flags, q_ref, k_ref, v_ref, across, far, low, high, near_low, near_high, *refs):
    sum_ref, weight_ref, top_ref = refs[:3]
    scratch = refs[3:6]
    rows = q_ref.shape[0]
    even = flags[6] > 0
    spreads = spreads_for(rows, (1, 2, 3), scratch[2])
    for head in range(q_ref.shape[1] // HEAD_DIM):
        lanes, work = start_head(head, q_ref, spreads, flags, scratch)
        work.take(k_ref[:, lanes], v_ref[:, lanes], 0, None)
        for ref, flag in ((low, 3), (high, 4)):
            work.take(ref[:256, lanes], ref[256:, lanes], 2, flag)
        near = [
            jnp.where(
                even,
                near_low[part * 128 : (part + 1) * 128, lanes],
                near_high[part * 128 : (part + 1) * 128, lanes],
            )
            for part in range(2)
        ]
        work.take(near[0], near[1], 3, 9)
        for ref, flag in ((across, None), (far, 10)):
            work.take(ref[:128, lanes], ref[128:, lanes], 1, flag)
        top = work.top()
        numerator, denominator = work.sums(top)
        sum_ref[:, lanes] = numerator
        weight_ref[:, lanes] = denominator
        top_ref[:, lanes] = jnp.broadcast_to(top, (rows, HEAD_DIM))


def late_kernel(flags, q_ref, sum_ref, weight_ref, top_ref, low, high, skew, skew_across, *refs):
    third_from, left_from, right_from, left_wrap, right_wrap, out_ref = refs[:6]
    scratch = refs[6:9]
    third, left, right, arrived = refs[9:13]
    copies = [pltpu.make_async_copy(third_from, third, arrived.at[0])]
    copies[0].start()
    sides = ((left_from, left_wrap, left, 13), (right_from, right_wrap, right, 14))
    for index, (inner_from, wrap_from, target, flag) in enumerate(sides, 1):
        inner = pltpu.make_async_copy(inner_from, target, arrived.at[index])
        wrapped = pltpu.make_async_copy(wrap_from, target, arrived.at[index])
        lax.cond(flags[flag] > 0, wrapped.start, inner.start)
        copies.append(inner)

    beside_left = flags[2] > 0
    half = mean_matrix(128, 2)
    spreads = spreads_for(q_ref.shape[0], (1, 3), scratch[2])
    for head in range(q_ref.shape[1] // HEAD_DIM):
        lanes, work = start_head(head, q_ref, spreads, flags, scratch)
        for ref, flag in ((low, 5), (high, 7)):
            work.take(ref[:128, lanes], ref[128:, lanes], 3, flag)
        if head == 0:
            for copy in copies:
                copy.wait()
        gathered = [
            jnp.concatenate(
                [
                    ref[base + part * 32 : base + (part + 1) * 32, lanes]
                    for ref, base in ((skew, 0), (skew_across, 0), (third, 256), (third, 320))
                ],
                0,
            )
            for part in range(2)
        ]
        work.take(gathered[0], gathered[1], 3, 8)
        work.take(third[:128, lanes], third[128:256, lanes], 1, 11)
        for ref, flag in ((left, 0), (right, 1)):
            work.take(ref[:256, lanes], ref[256:, lanes], 0, flag)
        fourth = [
            dot(
                half,
                jnp.where(
                    beside_left,
                    left[part * 256 : (part + 1) * 256, lanes],
                    right[part * 256 : (part + 1) * 256, lanes],
                ),
            ).astype(jnp.bfloat16)
            for part in range(2)
        ]
        work.take(fourth[0], fourth[1], 1, 12)
        early = top_ref[:, lanes]
        top = jnp.maximum(early[:, :1], work.top())
        kept = jnp.exp2(early - top)
        numerator, denominator = work.sums(top)
        numerator = sum_ref[:, lanes] * kept + numerator
        denominator = weight_ref[:, lanes] * kept + denominator
        out_ref[:, lanes] = (numerator / denominator).astype(jnp.bfloat16)


def heads_call(kernel, flags, tensors, outs, scratch, limit, flops, away=()):
    whole = pl.BlockSpec(memory_space=pltpu.VMEM)
    several = len(outs) > 1
    return pl.pallas_call(
        kernel,
        in_specs=[pl.BlockSpec(memory_space=pltpu.SMEM)]
        + [pl.BlockSpec(memory_space=pl.ANY) if i in away else whole for i in range(len(tensors))],
        out_specs=(whole,) * len(outs) if several else whole,
        out_shape=tuple(outs) if several else outs[0],
        scratch_shapes=scratch,
        compiler_params=pltpu.CompilerParams(vmem_limit_bytes=limit * MIB),
        cost_estimate=pl.CostEstimate(flops=flops, bytes_accessed=6 * 10**6, transcendentals=0),
    )(flags, *tensors)


def scratch_for(rows):
    return [
        pltpu.VMEM((2, rows, KEYS), jnp.float32),
        pltpu.VMEM((2, rows, KEYS), jnp.bfloat16),
        pltpu.VMEM((2, KEYS, 2 * HEAD_DIM), jnp.bfloat16),
    ]


def attend_main(flags, tensors):
    rows, width = tensors[0].shape
    outs = [jax.ShapeDtypeStruct((rows, width), jnp.float32)] * 3
    scratch = scratch_for(rows)
    return heads_call(main_kernel, flags, tensors, outs, scratch, 24, 2 * 10**9)


def attend_late(flags, tensors):
    rows, width = tensors[0].shape
    outs = [jax.ShapeDtypeStruct((rows, width), jnp.bfloat16)]
    away = (8, 9, 10, 11, 12)
    scratch = scratch_for(rows) + [pltpu.VMEM(tensors[i].shape, jnp.bfloat16) for i in away[:3]]
    scratch.append(pltpu.SemaphoreType.DMA((3,)))
    return heads_call(late_kernel, flags, tensors, outs, scratch, 24, 2 * 10**9, away)


def project_kernel(column, a_ref, b_ref, wa_ref, wb_ref, out_ref):
    total = dot(a_ref[...], wa_ref[...]) + dot(b_ref[...], wb_ref[...])
    out_ref[...] = total.astype(out_ref.dtype)


def project(column, own, peer, own_weight, peer_weight, dtype):
    rows, width = own.shape
    block = pl.BlockSpec((rows, width), lambda i, c: (0, 0))
    weight = pl.BlockSpec((width, width), lambda i, c: (0, c[0]))
    return pl.pallas_call(
        project_kernel,
        grid_spec=pltpu.PrefetchScalarGridSpec(
            num_scalar_prefetch=1,
            grid=(1,),
            in_specs=[block, block, weight, weight],
            out_specs=block,
        ),
        out_shape=jax.ShapeDtypeStruct((rows, width), dtype),
        compiler_params=pltpu.CompilerParams(vmem_limit_bytes=12 * MIB),
        cost_estimate=pl.CostEstimate(flops=10**9, bytes_accessed=10**6, transcendentals=0),
    )(column, own, peer, own_weight, peer_weight)


def layer(queries, key_rows, value_rows, out_weight):
    device = lax.axis_index("seq")
    head = lax.axis_index("head")
    last = lax.axis_size("seq") - 1
    lines = lax.axis_size("seq") // 4
    line = device // 4
    spot = device % 4
    even = line % 2 == 0

    raw, own_one, own_two, own_three = coarse(key_rows, value_rows)
    across = seq_permute(own_one, lambda i: i ^ 2)
    skew = seq_permute(own_three, lambda i: i + 12 if i // 4 % 2 == 0 else i - 12)
    peer_weight = head_permute(out_weight, 1)
    two_half = small(half_kernel, own_two, across)
    two_beside = seq_permute(two_half, lambda i: i ^ 1)
    skew_across = seq_permute(skew, lambda i: i ^ 2)
    far = seq_permute(across, lambda i: i + 4 if i % 4 < 2 else i - 4)
    left = seq_permute(raw, lambda i: i + 1 if i % 4 < 3 else -1)
    right = seq_permute(raw, lambda i: i - 1 if i % 4 > 0 else -1)
    two_block = small(pack_kernel, two_half, two_beside, rows=(512,))
    two_low = seq_permute(two_block, lambda i: i + 4)
    two_high = seq_permute(two_block, lambda i: i - 4)
    outer = (spot == 0) | (spot == 3)
    handed = hand(outer.astype(jnp.int32).reshape(1), far, across, skew, skew_across)
    third = seq_permute(handed, lambda i: i ^ 1)
    left_wrap = seq_permute(raw, lambda i: i + 1 if i % 4 == 3 else -1)
    right_wrap = seq_permute(raw, lambda i: i - 1 if i % 4 == 0 else -1)
    near_low = small(halve_kernel, two_low)
    near_high = small(halve_kernel, two_high)
    three_low = seq_permute(near_low, lambda i: i + 4)
    three_high = seq_permute(near_high, lambda i: i - 4)

    far_ok = jnp.where(spot < 2, line > 0, line < lines - 1)
    flags = jnp.stack(
        [
            device > 0,
            device < last,
            spot % 2 == 0,
            line > 0,
            line < lines - 1,
            line >= 2,
            even,
            line < lines - 2,
            jnp.where(even, line < lines - 3, line >= 3),
            jnp.where(even, line > 0, line < lines - 1),
            far_ok,
            outer | far_ok,
            jnp.logical_not(outer) | far_ok,
            spot == 0,
            spot == 3,
        ]
    ).astype(jnp.int32)
    tensors = [queries, key_rows, value_rows, across, far, two_low, two_high]
    partial = attend_main(flags, tensors + [near_low, near_high])
    tensors = [queries, *partial, three_low, three_high, skew, skew_across]
    tensors += [third, left, right, left_wrap, right_wrap]
    attended = attend_late(flags, tensors)
    peer = head_permute(attended, 1)
    here_column, away_column = head.reshape(1), (head ^ 2).reshape(1)
    weights = (out_weight, peer_weight)
    away = project(away_column, attended, peer, *weights, jnp.bfloat16)
    arrived = head_permute(away, 2)
    here = project(here_column, attended, peer, *weights, jnp.float32)
    return (here + arrived.astype(jnp.float32)).astype(jnp.bfloat16)


def solution(mesh):
    in_specs = (P("seq", "head"), P("seq", "head"), P("seq", "head"), P("head", None))
    out_specs = P("seq", "head")
    return jax.shard_map(layer, mesh=mesh, in_specs=in_specs, out_specs=out_specs, check_vma=False)
```

```python
import jax
import jax.numpy as jnp
from jax import lax
from jax.experimental import pallas as pl
from jax.experimental.pallas import tpu as pltpu
from jax.sharding import PartitionSpec as P


HEAD_DIM = 128
LOG2E = 1.4426950408889634
MIB = 1024 * 1024


def in_hbm(values):
    return [pltpu.with_memory_space_constraint(value, pltpu.HBM) for value in values]


def seq_permute(value, target_of):
    count = lax.axis_size("seq")
    pairs = [(i, target_of(i)) for i in range(count)]
    pairs = [(i, j) for i, j in pairs if 0 <= j < count]
    return lax.ppermute(value, "seq", pairs)


def head_permute(value, bit):
    count = lax.axis_size("head")
    return lax.ppermute(value, "head", [(i, i ^ bit) for i in range(count)])


def mean_matrix(rows, factor):
    row = lax.broadcasted_iota(jnp.int32, (rows, rows * factor), 0)
    col = lax.broadcasted_iota(jnp.int32, (rows, rows * factor), 1)
    return jnp.where(col // factor == row, 1.0 / factor, 0.0).astype(jnp.bfloat16)


def spread_mean_matrix(rows, factor):
    row = lax.broadcasted_iota(jnp.int32, (rows, rows), 0)
    col = lax.broadcasted_iota(jnp.int32, (rows, rows), 1)
    return jnp.where(col // factor == row // factor, 1.0 / factor, 0.0).astype(jnp.bfloat16)


def dot(left, right):
    return jnp.dot(left, right, preferred_element_type=jnp.float32)


def dot_t(left, right):
    return lax.dot_general(left, right, (((1,), (1,)), ((), ())), preferred_element_type=jnp.float32)


def coarse_kernel(k_ref, v_ref, raw_ref, one_ref, two_ref, three_ref):
    half, quarter, eighth = mean_matrix(128, 2), mean_matrix(64, 4), mean_matrix(32, 8)
    for index, ref in enumerate((k_ref, v_ref)):
        value = ref[...]
        raw_ref[index * 256 : (index + 1) * 256] = value
        one_ref[index * 128 : (index + 1) * 128] = dot(half, value).astype(jnp.bfloat16)
        two_ref[index * 64 : (index + 1) * 64] = dot(quarter, value).astype(jnp.bfloat16)
        three_ref[index * 32 : (index + 1) * 32] = dot(eighth, value).astype(jnp.bfloat16)


def coarse(k, v):
    width = k.shape[1]
    return pl.pallas_call(
        coarse_kernel,
        out_shape=(
            jax.ShapeDtypeStruct((512, width), jnp.bfloat16),
            jax.ShapeDtypeStruct((256, width), jnp.bfloat16),
            jax.ShapeDtypeStruct((128, width), jnp.bfloat16),
            jax.ShapeDtypeStruct((64, width), jnp.bfloat16),
        ),
        compiler_params=pltpu.CompilerParams(vmem_limit_bytes=8 * MIB),
        cost_estimate=pl.CostEstimate(flops=10**8, bytes_accessed=10**6, transcendentals=0),
        name="coarse",
    )(*in_hbm((k, v)))


def half_kernel(two_ref, one_ref, out_ref):
    half = mean_matrix(64, 2)
    for part in range(2):
        base = part * 128
        out_ref[base : base + 64] = two_ref[part * 64 : (part + 1) * 64]
        out_ref[base + 64 : base + 128] = dot(half, one_ref[base : base + 128]).astype(jnp.bfloat16)


def halve_kernel(block_ref, out_ref):
    half = mean_matrix(128, 2)
    for part in range(2):
        out_ref[part * 128 : (part + 1) * 128] = dot(
            half, block_ref[part * 256 : (part + 1) * 256]
        ).astype(jnp.bfloat16)


def pack_kernel(a_ref, b_ref, out_ref):
    for part in range(2):
        for index, ref in enumerate((a_ref, b_ref)):
            start = part * 256 + index * 128
            out_ref[start : start + 128] = ref[part * 128 : (part + 1) * 128]


def hand_kernel(outer, far_ref, across_ref, skew_ref, skew_across_ref, out_ref):
    out_ref[:256] = jnp.where(outer[0] > 0, far_ref[...], across_ref[...])
    out_ref[256:320] = skew_ref[...]
    out_ref[320:384] = skew_across_ref[...]


def hand(outer, far, across, skew, skew_across):
    whole = pl.BlockSpec(memory_space=pltpu.VMEM)
    return pl.pallas_call(
        hand_kernel,
        in_specs=[pl.BlockSpec(memory_space=pltpu.SMEM)] + [whole] * 4,
        out_specs=whole,
        out_shape=jax.ShapeDtypeStruct((384, far.shape[1]), far.dtype),
        compiler_params=pltpu.CompilerParams(vmem_limit_bytes=4 * MIB),
        cost_estimate=pl.CostEstimate(flops=10**8, bytes_accessed=10**6, transcendentals=0),
        name="hand",
    )(outer, far, across, skew, skew_across)


def small(kernel, *operands, rows=(256,)):
    width, dtype = operands[0].shape[1], operands[0].dtype
    shapes = tuple(jax.ShapeDtypeStruct((count, width), dtype) for count in rows)
    return pl.pallas_call(
        kernel,
        out_shape=shapes if len(rows) > 1 else shapes[0],
        compiler_params=pltpu.CompilerParams(vmem_limit_bytes=4 * MIB),
        cost_estimate=pl.CostEstimate(flops=10**8, bytes_accessed=10**6, transcendentals=0),
    )(*operands)


LATE = 2 * 128
KEYS = 768 + 3 * 512 - LATE
SCALE = LOG2E * HEAD_DIM**-0.5


def bias(flags, index):
    return jnp.where(flags[index] > 0, 0.0, -jnp.inf)


def main_kernel(flags, q_ref, *refs):
    across, far = refs[4:6]
    twos = refs[7:9]
    skews = refs[9:11]
    nears = refs[11:13]
    wraps = refs[13:15]
    sum_ref, weight_ref, top_ref = refs[15:18]
    scores, weights, values, left, right, third, k_ref, v_ref, arrived = refs[18:27]
    copies = [
        pltpu.make_async_copy(source, target, arrived.at[index])
        for index, (source, target) in enumerate(
            (
                (refs[2], left),
                (refs[3], right),
                (refs[6], third),
                (refs[0], k_ref),
                (refs[1], v_ref),
            )
        )
    ]
    for copy in copies[2:]:
        copy.start()
    for index, flag in ((0, 13), (1, 14)):
        wrapped = pltpu.make_async_copy(
            wraps[index], (left, right)[index], arrived.at[index]
        )

        lax.cond(flags[flag] > 0, wrapped.start, copies[index].start)

    rows = q_ref.shape[0]
    even = flags[6] > 0
    beside_left = flags[2] > 0
    half = mean_matrix(128, 2)
    spreads = [spread_mean_matrix(rows, 2**level) for level in range(1, 4)]
    for slot in range(2):
        values[slot, :, HEAD_DIM:] = jnp.ones((KEYS, HEAD_DIM), jnp.bfloat16)

    for head in range(q_ref.shape[1] // HEAD_DIM):
        slot = head % 2
        lanes = slice(head * HEAD_DIM, (head + 1) * HEAD_DIM)

        def rows_of(ref, start, count):
            return ref[start : start + count, lanes]

        def either(flag, first, second, start, count):
            return jnp.where(flag, rows_of(first, start, count), rows_of(second, start, count))

        query = rows_of(q_ref, 0, rows)
        queries = [query] + [dot(spread, query).astype(jnp.bfloat16) for spread in spreads]
        largest = None
        spans = []

        def take(keys, vals, level, flag):
            nonlocal largest
            start = spans[-1][0] + spans[-1][1] if spans else 0
            count = keys.shape[0]
            part = dot_t(queries[level], keys)
            if flag is not None:
                part = part + bias(flags, flag)
            scores[slot, :, start : start + count] = part
            values[slot, start : start + count, :HEAD_DIM] = vals
            for column in range(0, count, 128):
                piece = part[:, column : column + 128]
                largest = piece if largest is None else jnp.maximum(largest, piece)
            spans.append((start, count, level))

        for index, ref in enumerate(twos):
            take(rows_of(ref, 0, 256), rows_of(ref, 256, 256), 2, 3 + index)
        near = [either(even, nears[0], nears[1], part * 128, 128) for part in range(2)]
        take(near[0], near[1], 3, 9)
        for ref, flag in ((across, None), (far, 10)):
            take(rows_of(ref, 0, 128), rows_of(ref, 128, 128), 1, flag)
        if head == 0:
            for copy in copies:
                copy.wait()
        take(rows_of(k_ref, 0, 256), rows_of(v_ref, 0, 256), 0, None)
        take(rows_of(third, 0, 128), rows_of(third, 128, 128), 1, 11)
        skew = [
            jnp.concatenate(
                [
                    rows_of(skews[0], part * 32, 32),
                    rows_of(skews[1], part * 32, 32),
                    rows_of(third, 256 + part * 32, 32),
                    rows_of(third, 320 + part * 32, 32),
                ],
                0,
            )
            for part in range(2)
        ]
        take(skew[0], skew[1], 3, 8)
        for index, ref in enumerate((left, right)):
            take(rows_of(ref, 0, 256), rows_of(ref, 256, 256), 0, index)
        fourth = [
            dot(half, either(beside_left, left, right, part * 256, 256)).astype(jnp.bfloat16)
            for part in range(2)
        ]
        take(fourth[0], fourth[1], 1, 12)
        top = jnp.max(largest, axis=1, keepdims=True) * SCALE
        for start, count, level in spans:
            shifted = scores[slot, :, start : start + count] * SCALE - (top - level)
            weights[slot, :, start : start + count] = jnp.exp2(shifted).astype(jnp.bfloat16)
        total = dot(weights[slot], values[slot])
        sum_ref[:, lanes] = total[:, :HEAD_DIM]
        weight_ref[:, lanes] = total[:, HEAD_DIM:]
        top_ref[:, lanes] = jnp.broadcast_to(top, (rows, HEAD_DIM))


def late_kernel(flags, q_ref, sum_ref, weight_ref, top_ref, low, high, out_ref, values):
    rows = q_ref.shape[0]
    spread = spread_mean_matrix(rows, 8)
    for slot in range(2):
        values[slot, :, HEAD_DIM:] = jnp.ones((LATE, HEAD_DIM), jnp.bfloat16)
    for head in range(q_ref.shape[1] // HEAD_DIM):
        slot = head % 2
        lanes = slice(head * HEAD_DIM, (head + 1) * HEAD_DIM)
        query = dot(spread, q_ref[:, lanes]).astype(jnp.bfloat16)
        parts = []
        for index, (ref, flag) in enumerate(((low, 5), (high, 7))):
            parts.append(dot_t(query, ref[:128, lanes]) + bias(flags, flag))
            values[slot, index * 128 : (index + 1) * 128, :HEAD_DIM] = ref[128:, lanes]
        early = top_ref[:, lanes]
        top = jnp.max(jnp.maximum(parts[0], parts[1]), axis=1, keepdims=True) * SCALE
        top = jnp.maximum(early, top)
        kept = jnp.exp2(early - top)
        part = jnp.concatenate([jnp.exp2(p * SCALE - (top - 3.0)) for p in parts], 1)
        total = dot(part.astype(jnp.bfloat16), values[slot])
        numerator = sum_ref[:, lanes] * kept + total[:, :HEAD_DIM]
        denominator = weight_ref[:, lanes] * kept + total[:, HEAD_DIM:]
        out_ref[:, lanes] = (numerator / denominator).astype(jnp.bfloat16)


def heads_call(kernel, flags, tensors, outs, scratch, limit, flops, away=()):
    whole = pl.BlockSpec(memory_space=pltpu.VMEM)
    several = len(outs) > 1
    return pl.pallas_call(
        kernel,
        in_specs=[pl.BlockSpec(memory_space=pltpu.SMEM)]
        + [pl.BlockSpec(memory_space=pl.ANY) if i in away else whole for i in range(len(tensors))],
        out_specs=(whole,) * len(outs) if several else whole,
        out_shape=tuple(outs) if several else outs[0],
        scratch_shapes=scratch,
        compiler_params=pltpu.CompilerParams(vmem_limit_bytes=limit * MIB),
        cost_estimate=pl.CostEstimate(flops=flops, bytes_accessed=6 * 10**6, transcendentals=0),
    )(flags, *tensors)


def attend_main(flags, tensors):
    rows, width = tensors[0].shape
    outs = [jax.ShapeDtypeStruct((rows, width), jnp.float32)] * 3
    scratch = [
        pltpu.VMEM((2, rows, KEYS), jnp.float32),
        pltpu.VMEM((2, rows, KEYS), jnp.bfloat16),
        pltpu.VMEM((2, KEYS, 2 * HEAD_DIM), jnp.bfloat16),
    ]
    landed, away = (3, 4, 7, 1, 2), (3, 4, 7, 1, 2, 14, 15)
    scratch += [pltpu.VMEM(tensors[i].shape, jnp.bfloat16) for i in landed]
    scratch.append(pltpu.SemaphoreType.DMA((len(landed),)))
    return heads_call(main_kernel, flags, tensors, outs, scratch, 32, 3 * 10**9, away)


def attend_late(flags, tensors):
    rows, width = tensors[0].shape
    outs = [jax.ShapeDtypeStruct((rows, width), jnp.bfloat16)]
    scratch = [pltpu.VMEM((2, LATE, 2 * HEAD_DIM), jnp.bfloat16)]
    return heads_call(late_kernel, flags, tensors, outs, scratch, 16, 3 * 10**8)


def pick_kernel(columns, own_ref, peer_ref, out_ref):
    out_ref[:512] = own_ref[...]
    out_ref[512:] = peer_ref[...]


def pick(columns, own_weight, peer_weight):
    rows = own_weight.shape[0]
    source = pl.BlockSpec((rows, rows), lambda i, c: (0, c[i]))
    return pl.pallas_call(
        pick_kernel,
        grid_spec=pltpu.PrefetchScalarGridSpec(
            num_scalar_prefetch=1,
            grid=(2,),
            in_specs=[source, source],
            out_specs=pl.BlockSpec((2 * rows, rows), lambda i, c: (i, 0)),
        ),
        out_shape=jax.ShapeDtypeStruct((4 * rows, rows), own_weight.dtype),
        compiler_params=pltpu.CompilerParams(vmem_limit_bytes=12 * MIB),
        cost_estimate=pl.CostEstimate(flops=10**8, bytes_accessed=10**6, transcendentals=0),
        name="pick",
    )(columns, *in_hbm((own_weight, peer_weight)))


def own_kernel(own_ref, weight_ref, out_ref):
    out_ref[...] = dot(own_ref[...], weight_ref[:512])


def away_kernel(part_ref, peer_ref, weight_ref, out_ref):
    out_ref[...] = (part_ref[...] + dot(peer_ref[...], weight_ref[512:1024])).astype(jnp.bfloat16)


def here_kernel(own_ref, peer_ref, weight_ref, out_ref):
    out_ref[...] = dot(own_ref[...], weight_ref[1024:1536]) + dot(
        peer_ref[...], weight_ref[1536:]
    )


def project(kernel, operands, dtype):
    return pl.pallas_call(
        kernel,
        out_shape=jax.ShapeDtypeStruct(operands[0].shape, dtype),
        compiler_params=pltpu.CompilerParams(vmem_limit_bytes=8 * MIB),
        cost_estimate=pl.CostEstimate(flops=5 * 10**8, bytes_accessed=10**6, transcendentals=0),
    )(*operands)


def layer(queries, key_rows, value_rows, out_weight):
    device = lax.axis_index("seq")
    head = lax.axis_index("head")
    last = lax.axis_size("seq") - 1
    lines = lax.axis_size("seq") // 4
    line = device // 4
    spot = device % 4
    even = line % 2 == 0

    raw, own_one, own_two, own_three = coarse(key_rows, value_rows)
    across = seq_permute(own_one, lambda i: i ^ 2)
    skew = seq_permute(own_three, lambda i: i + 12 if i // 4 % 2 == 0 else i - 12)
    peer_weight = head_permute(out_weight, 1)
    weights = pick(jnp.stack([head ^ 2, head]), out_weight, peer_weight)
    two_half = small(half_kernel, own_two, across)
    two_beside = seq_permute(two_half, lambda i: i ^ 1)
    skew_across = seq_permute(skew, lambda i: i ^ 2)
    far = seq_permute(across, lambda i: i + 4 if i % 4 < 2 else i - 4)
    left = seq_permute(raw, lambda i: i + 1 if i % 4 < 3 else -1)
    right = seq_permute(raw, lambda i: i - 1 if i % 4 > 0 else -1)
    two_block = small(pack_kernel, two_half, two_beside, rows=(512,))
    two_low = seq_permute(two_block, lambda i: i + 4)
    two_high = seq_permute(two_block, lambda i: i - 4)
    outer = (spot == 0) | (spot == 3)
    handed = hand(outer.astype(jnp.int32).reshape(1), far, across, skew, skew_across)
    third = seq_permute(handed, lambda i: i ^ 1)
    left_wrap = seq_permute(raw, lambda i: i + 1 if i % 4 == 3 else -1)
    right_wrap = seq_permute(raw, lambda i: i - 1 if i % 4 == 0 else -1)
    near_low = small(halve_kernel, two_low)
    near_high = small(halve_kernel, two_high)
    three_low = seq_permute(near_low, lambda i: i + 4)
    three_high = seq_permute(near_high, lambda i: i - 4)

    far_ok = jnp.where(spot < 2, line > 0, line < lines - 1)
    flags = jnp.stack(
        [
            device > 0,
            device < last,
            spot % 2 == 0,
            line > 0,
            line < lines - 1,
            line >= 2,
            even,
            line < lines - 2,
            jnp.where(even, line < lines - 3, line >= 3),
            jnp.where(even, line > 0, line < lines - 1),
            far_ok,
            outer | far_ok,
            jnp.logical_not(outer) | far_ok,
            spot == 0,
            spot == 3,
        ]
    ).astype(jnp.int32)
    tensors = in_hbm([queries, key_rows, value_rows]) + [left, right, across, far, third]
    tensors += [two_low, two_high, skew, skew_across, near_low, near_high]
    tensors += [left_wrap, right_wrap]
    partial = attend_main(flags, tensors)
    attended = attend_late(flags, [queries, *partial, three_low, three_high])
    peer = head_permute(attended, 1)
    part = project(own_kernel, (attended, weights), jnp.float32)
    away = project(away_kernel, (part, peer, weights), jnp.bfloat16)
    arrived = head_permute(away, 2)
    here = project(here_kernel, (attended, peer, weights), jnp.float32)
    return (here + arrived.astype(jnp.float32)).astype(jnp.bfloat16)


def solution(mesh):
    in_specs = (P("seq", "head"), P("seq", "head"), P("seq", "head"), P("head", None))
    out_specs = P("seq", "head")
    return jax.shard_map(layer, mesh=mesh, in_specs=in_specs, out_specs=out_specs, check_vma=False)
```

```python
import jax
import jax.numpy as jnp
from jax import lax
from jax.experimental import pallas as pl
from jax.experimental.pallas import tpu as pltpu
from jax.sharding import PartitionSpec as P


HEAD_DIM = 128
LOG2E = 1.4426950408889634
MIB = 1024 * 1024


def in_hbm(values):
    return [pltpu.with_memory_space_constraint(value, pltpu.HBM) for value in values]


def seq_permute(value, target_of):
    count = lax.axis_size("seq")
    pairs = [(i, target_of(i)) for i in range(count)]
    pairs = [(i, j) for i, j in pairs if 0 <= j < count]
    return lax.ppermute(value, "seq", pairs)


def head_permute(value, bit):
    count = lax.axis_size("head")
    return lax.ppermute(value, "head", [(i, i ^ bit) for i in range(count)])


def mean_matrix(rows, factor):
    row = lax.broadcasted_iota(jnp.int32, (rows, rows * factor), 0)
    col = lax.broadcasted_iota(jnp.int32, (rows, rows * factor), 1)
    return jnp.where(col // factor == row, 1.0 / factor, 0.0).astype(jnp.bfloat16)


def spread_mean_matrix(rows, factor):
    row = lax.broadcasted_iota(jnp.int32, (rows, rows), 0)
    col = lax.broadcasted_iota(jnp.int32, (rows, rows), 1)
    return jnp.where(col // factor == row // factor, 1.0 / factor, 0.0).astype(jnp.bfloat16)


def dot(left, right):
    return jnp.dot(left, right, preferred_element_type=jnp.float32)


def dot_t(left, right):
    return lax.dot_general(left, right, (((1,), (1,)), ((), ())), preferred_element_type=jnp.float32)


def coarse_kernel(k_ref, v_ref, raw_ref, one_ref, two_ref, three_ref):
    half, quarter, eighth = mean_matrix(128, 2), mean_matrix(64, 4), mean_matrix(32, 8)
    for index, ref in enumerate((k_ref, v_ref)):
        value = ref[...]
        raw_ref[index * 256 : (index + 1) * 256] = value
        one_ref[index * 128 : (index + 1) * 128] = dot(half, value).astype(jnp.bfloat16)
        two_ref[index * 64 : (index + 1) * 64] = dot(quarter, value).astype(jnp.bfloat16)
        three_ref[index * 32 : (index + 1) * 32] = dot(eighth, value).astype(jnp.bfloat16)


def coarse(k, v):
    width = k.shape[1]
    return pl.pallas_call(
        coarse_kernel,
        out_shape=(
            jax.ShapeDtypeStruct((512, width), jnp.bfloat16),
            jax.ShapeDtypeStruct((256, width), jnp.bfloat16),
            jax.ShapeDtypeStruct((128, width), jnp.bfloat16),
            jax.ShapeDtypeStruct((64, width), jnp.bfloat16),
        ),
        compiler_params=pltpu.CompilerParams(vmem_limit_bytes=8 * MIB),
        cost_estimate=pl.CostEstimate(flops=10**8, bytes_accessed=10**6, transcendentals=0),
        name="coarse",
    )(*in_hbm((k, v)))


def half_kernel(two_ref, one_ref, out_ref):
    half = mean_matrix(64, 2)
    for part in range(2):
        base = part * 128
        out_ref[base : base + 64] = two_ref[part * 64 : (part + 1) * 64]
        out_ref[base + 64 : base + 128] = dot(half, one_ref[base : base + 128]).astype(jnp.bfloat16)


def halve_kernel(block_ref, out_ref):
    half = mean_matrix(128, 2)
    for part in range(2):
        out_ref[part * 128 : (part + 1) * 128] = dot(
            half, block_ref[part * 256 : (part + 1) * 256]
        ).astype(jnp.bfloat16)


def pack_kernel(a_ref, b_ref, out_ref):
    for part in range(2):
        for index, ref in enumerate((a_ref, b_ref)):
            start = part * 256 + index * 128
            out_ref[start : start + 128] = ref[part * 128 : (part + 1) * 128]


def hand_kernel(outer, far_ref, across_ref, skew_ref, skew_across_ref, out_ref):
    out_ref[:256] = jnp.where(outer[0] > 0, far_ref[...], across_ref[...])
    out_ref[256:320] = skew_ref[...]
    out_ref[320:384] = skew_across_ref[...]


def hand(outer, far, across, skew, skew_across):
    whole = pl.BlockSpec(memory_space=pltpu.VMEM)
    return pl.pallas_call(
        hand_kernel,
        in_specs=[pl.BlockSpec(memory_space=pltpu.SMEM)] + [whole] * 4,
        out_specs=whole,
        out_shape=jax.ShapeDtypeStruct((384, far.shape[1]), far.dtype),
        compiler_params=pltpu.CompilerParams(vmem_limit_bytes=4 * MIB),
        cost_estimate=pl.CostEstimate(flops=10**8, bytes_accessed=10**6, transcendentals=0),
        name="hand",
    )(outer, far, across, skew, skew_across)


def small(kernel, *operands, rows=(256,)):
    width, dtype = operands[0].shape[1], operands[0].dtype
    shapes = tuple(jax.ShapeDtypeStruct((count, width), dtype) for count in rows)
    return pl.pallas_call(
        kernel,
        out_shape=shapes if len(rows) > 1 else shapes[0],
        compiler_params=pltpu.CompilerParams(vmem_limit_bytes=4 * MIB),
        cost_estimate=pl.CostEstimate(flops=10**8, bytes_accessed=10**6, transcendentals=0),
    )(*operands)


LATE = 2 * 128
KEYS = 768 + 3 * 512 - LATE
SCALE = LOG2E * HEAD_DIM**-0.5


def bias(flags, index):
    return jnp.where(flags[index] > 0, 0.0, -jnp.inf)


def main_kernel(flags, q_ref, *refs):
    k_ref, v_ref = refs[0:2]
    across, far = refs[4:6]
    twos = refs[7:9]
    skews = refs[9:11]
    nears = refs[11:13]
    wraps = refs[13:15]
    sum_ref, weight_ref, top_ref = refs[15:18]
    scores, weights, values, left, right, third, arrived = refs[18:25]
    copies = [
        pltpu.make_async_copy(source, target, arrived.at[index])
        for index, (source, target) in enumerate(
            ((refs[2], left), (refs[3], right), (refs[6], third))
        )
    ]
    copies[2].start()
    for index, flag in ((0, 13), (1, 14)):
        wrapped = pltpu.make_async_copy(
            wraps[index], (left, right)[index], arrived.at[index]
        )

        lax.cond(flags[flag] > 0, wrapped.start, copies[index].start)

    rows = q_ref.shape[0]
    even = flags[6] > 0
    beside_left = flags[2] > 0
    half = mean_matrix(128, 2)
    spreads = [spread_mean_matrix(rows, 2**level) for level in range(1, 4)]
    for slot in range(2):
        values[slot, :, HEAD_DIM:] = jnp.ones((KEYS, HEAD_DIM), jnp.bfloat16)

    for head in range(q_ref.shape[1] // HEAD_DIM):
        slot = head % 2
        lanes = slice(head * HEAD_DIM, (head + 1) * HEAD_DIM)

        def rows_of(ref, start, count):
            return ref[start : start + count, lanes]

        def either(flag, first, second, start, count):
            return jnp.where(flag, rows_of(first, start, count), rows_of(second, start, count))

        query = rows_of(q_ref, 0, rows)
        queries = [query] + [dot(spread, query).astype(jnp.bfloat16) for spread in spreads]
        largest = None
        spans = []

        def take(keys, vals, level, flag):
            nonlocal largest
            start = spans[-1][0] + spans[-1][1] if spans else 0
            count = keys.shape[0]
            part = dot_t(queries[level], keys)
            if flag is not None:
                part = part + bias(flags, flag)
            scores[slot, :, start : start + count] = part
            values[slot, start : start + count, :HEAD_DIM] = vals
            for column in range(0, count, 128):
                piece = part[:, column : column + 128]
                largest = piece if largest is None else jnp.maximum(largest, piece)
            spans.append((start, count, level))

        take(rows_of(k_ref, 0, 256), rows_of(v_ref, 0, 256), 0, None)
        for index, ref in enumerate(twos):
            take(rows_of(ref, 0, 256), rows_of(ref, 256, 256), 2, 3 + index)
        near = [either(even, nears[0], nears[1], part * 128, 128) for part in range(2)]
        take(near[0], near[1], 3, 9)
        for ref, flag in ((across, None), (far, 10)):
            take(rows_of(ref, 0, 128), rows_of(ref, 128, 128), 1, flag)
        if head == 0:
            for copy in copies:
                copy.wait()
        take(rows_of(third, 0, 128), rows_of(third, 128, 128), 1, 11)
        skew = [
            jnp.concatenate(
                [
                    rows_of(skews[0], part * 32, 32),
                    rows_of(skews[1], part * 32, 32),
                    rows_of(third, 256 + part * 32, 32),
                    rows_of(third, 320 + part * 32, 32),
                ],
                0,
            )
            for part in range(2)
        ]
        take(skew[0], skew[1], 3, 8)
        for index, ref in enumerate((left, right)):
            take(rows_of(ref, 0, 256), rows_of(ref, 256, 256), 0, index)
        fourth = [
            dot(half, either(beside_left, left, right, part * 256, 256)).astype(jnp.bfloat16)
            for part in range(2)
        ]
        take(fourth[0], fourth[1], 1, 12)
        top = jnp.max(largest, axis=1, keepdims=True) * SCALE
        for start, count, level in spans:
            shifted = scores[slot, :, start : start + count] * SCALE - (top - level)
            weights[slot, :, start : start + count] = jnp.exp2(shifted).astype(jnp.bfloat16)
        total = dot(weights[slot], values[slot])
        sum_ref[:, lanes] = total[:, :HEAD_DIM]
        weight_ref[:, lanes] = total[:, HEAD_DIM:]
        top_ref[:, lanes] = jnp.broadcast_to(top, (rows, HEAD_DIM))


def late_kernel(flags, q_ref, sum_ref, weight_ref, top_ref, low, high, out_ref, values):
    rows = q_ref.shape[0]
    spread = spread_mean_matrix(rows, 8)
    for slot in range(2):
        values[slot, :, HEAD_DIM:] = jnp.ones((LATE, HEAD_DIM), jnp.bfloat16)
    for head in range(q_ref.shape[1] // HEAD_DIM):
        slot = head % 2
        lanes = slice(head * HEAD_DIM, (head + 1) * HEAD_DIM)
        query = dot(spread, q_ref[:, lanes]).astype(jnp.bfloat16)
        parts = []
        for index, (ref, flag) in enumerate(((low, 5), (high, 7))):
            parts.append(dot_t(query, ref[:128, lanes]) + bias(flags, flag))
            values[slot, index * 128 : (index + 1) * 128, :HEAD_DIM] = ref[128:, lanes]
        early = top_ref[:, lanes]
        top = jnp.max(jnp.maximum(parts[0], parts[1]), axis=1, keepdims=True) * SCALE
        top = jnp.maximum(early, top)
        kept = jnp.exp2(early - top)
        part = jnp.concatenate([jnp.exp2(p * SCALE - (top - 3.0)) for p in parts], 1)
        total = dot(part.astype(jnp.bfloat16), values[slot])
        numerator = sum_ref[:, lanes] * kept + total[:, :HEAD_DIM]
        denominator = weight_ref[:, lanes] * kept + total[:, HEAD_DIM:]
        out_ref[:, lanes] = (numerator / denominator).astype(jnp.bfloat16)


def heads_call(kernel, flags, tensors, outs, scratch, limit, flops, away=()):
    whole = pl.BlockSpec(memory_space=pltpu.VMEM)
    several = len(outs) > 1
    return pl.pallas_call(
        kernel,
        in_specs=[pl.BlockSpec(memory_space=pltpu.SMEM)]
        + [pl.BlockSpec(memory_space=pl.ANY) if i in away else whole for i in range(len(tensors))],
        out_specs=(whole,) * len(outs) if several else whole,
        out_shape=tuple(outs) if several else outs[0],
        scratch_shapes=scratch,
        compiler_params=pltpu.CompilerParams(vmem_limit_bytes=limit * MIB),
        cost_estimate=pl.CostEstimate(flops=flops, bytes_accessed=6 * 10**6, transcendentals=0),
    )(flags, *tensors)


def attend_main(flags, tensors):
    rows, width = tensors[0].shape
    outs = [jax.ShapeDtypeStruct((rows, width), jnp.float32)] * 3
    scratch = [
        pltpu.VMEM((2, rows, KEYS), jnp.float32),
        pltpu.VMEM((2, rows, KEYS), jnp.bfloat16),
        pltpu.VMEM((2, KEYS, 2 * HEAD_DIM), jnp.bfloat16),
    ]
    landed, away = (3, 4, 7), (3, 4, 7, 14, 15)
    scratch += [pltpu.VMEM(tensors[i].shape, jnp.bfloat16) for i in landed]
    scratch.append(pltpu.SemaphoreType.DMA((len(landed),)))
    return heads_call(main_kernel, flags, tensors, outs, scratch, 32, 3 * 10**9, away)


def attend_late(flags, tensors):
    rows, width = tensors[0].shape
    outs = [jax.ShapeDtypeStruct((rows, width), jnp.bfloat16)]
    scratch = [pltpu.VMEM((2, LATE, 2 * HEAD_DIM), jnp.bfloat16)]
    return heads_call(late_kernel, flags, tensors, outs, scratch, 16, 3 * 10**8)


def project_kernel(column, a_ref, b_ref, wa_ref, wb_ref, out_ref):
    total = dot(a_ref[...], wa_ref[...]) + dot(b_ref[...], wb_ref[...])
    out_ref[...] = total.astype(out_ref.dtype)


def project(column, own, peer, own_weight, peer_weight, dtype):
    rows, width = own.shape
    block = pl.BlockSpec((rows, width), lambda i, c: (0, 0))
    weight = pl.BlockSpec((width, width), lambda i, c: (0, c[0]))
    return pl.pallas_call(
        project_kernel,
        grid_spec=pltpu.PrefetchScalarGridSpec(
            num_scalar_prefetch=1,
            grid=(1,),
            in_specs=[block, block, weight, weight],
            out_specs=block,
        ),
        out_shape=jax.ShapeDtypeStruct((rows, width), dtype),
        compiler_params=pltpu.CompilerParams(vmem_limit_bytes=12 * MIB),
        cost_estimate=pl.CostEstimate(flops=10**9, bytes_accessed=10**6, transcendentals=0),
    )(column, own, peer, own_weight, peer_weight)


def layer(queries, key_rows, value_rows, out_weight):
    device = lax.axis_index("seq")
    head = lax.axis_index("head")
    last = lax.axis_size("seq") - 1
    lines = lax.axis_size("seq") // 4
    line = device // 4
    spot = device % 4
    even = line % 2 == 0

    raw, own_one, own_two, own_three = coarse(key_rows, value_rows)
    across = seq_permute(own_one, lambda i: i ^ 2)
    skew = seq_permute(own_three, lambda i: i + 12 if i // 4 % 2 == 0 else i - 12)
    peer_weight = head_permute(out_weight, 1)
    two_half = small(half_kernel, own_two, across)
    two_beside = seq_permute(two_half, lambda i: i ^ 1)
    skew_across = seq_permute(skew, lambda i: i ^ 2)
    far = seq_permute(across, lambda i: i + 4 if i % 4 < 2 else i - 4)
    left = seq_permute(raw, lambda i: i + 1 if i % 4 < 3 else -1)
    right = seq_permute(raw, lambda i: i - 1 if i % 4 > 0 else -1)
    two_block = small(pack_kernel, two_half, two_beside, rows=(512,))
    two_low = seq_permute(two_block, lambda i: i + 4)
    two_high = seq_permute(two_block, lambda i: i - 4)
    outer = (spot == 0) | (spot == 3)
    handed = hand(outer.astype(jnp.int32).reshape(1), far, across, skew, skew_across)
    third = seq_permute(handed, lambda i: i ^ 1)
    left_wrap = seq_permute(raw, lambda i: i + 1 if i % 4 == 3 else -1)
    right_wrap = seq_permute(raw, lambda i: i - 1 if i % 4 == 0 else -1)
    near_low = small(halve_kernel, two_low)
    near_high = small(halve_kernel, two_high)
    three_low = seq_permute(near_low, lambda i: i + 4)
    three_high = seq_permute(near_high, lambda i: i - 4)

    far_ok = jnp.where(spot < 2, line > 0, line < lines - 1)
    flags = jnp.stack(
        [
            device > 0,
            device < last,
            spot % 2 == 0,
            line > 0,
            line < lines - 1,
            line >= 2,
            even,
            line < lines - 2,
            jnp.where(even, line < lines - 3, line >= 3),
            jnp.where(even, line > 0, line < lines - 1),
            far_ok,
            outer | far_ok,
            jnp.logical_not(outer) | far_ok,
            spot == 0,
            spot == 3,
        ]
    ).astype(jnp.int32)
    tensors = [queries, key_rows, value_rows, left, right, across, far, third]
    tensors += [two_low, two_high, skew, skew_across, near_low, near_high]
    tensors += [left_wrap, right_wrap]
    partial = attend_main(flags, tensors)
    attended = attend_late(flags, [queries, *partial, three_low, three_high])
    peer = head_permute(attended, 1)
    here_column, away_column = head.reshape(1), (head ^ 2).reshape(1)
    weights = (out_weight, peer_weight)
    away = project(away_column, attended, peer, *weights, jnp.bfloat16)
    arrived = head_permute(away, 2)
    here = project(here_column, attended, peer, *weights, jnp.float32)
    return (here + arrived.astype(jnp.float32)).astype(jnp.bfloat16)


def solution(mesh):
    in_specs = (P("seq", "head"), P("seq", "head"), P("seq", "head"), P("head", None))
    out_specs = P("seq", "head")
    return jax.shard_map(layer, mesh=mesh, in_specs=in_specs, out_specs=out_specs, check_vma=False)
```
